32 devices in a mesh: rows: 8 (over y, x, core), sub: 4 (over z).
Axes of the slice: x: 2, y: 2, z: 4, core: 2. Of those that a mesh axis runs over, the one named last changes fastest.
Arguments:
- u_fem: float32 [120, 524288], P(None, ('rows', 'sub')), may hold values from -600 to 600
- resid_fem: float32 [1, 524288], P(None, ('rows', 'sub')), may hold values from -60 to 60
- slot_map: int32 [32, 32], P(('rows', 'sub')), may hold values from 0 to 31, as said below
- restart: float32 [120, 40], replicated, may hold values from -0.5 to 0.5
- coeff: float32 [3, 120, 120], P(None, None, 'sub'), may hold values from -6 to 6
Outputs:
- new_basis: float32 [40, 524288], P(None, ('rows', 'sub'))
- next_vector: float32 [1, 524288], P(None, ('rows', 'sub'))
- new_coeff: float32 [3, 40, 120], replicated
The draws below stay inside these ranges and needn't reach their ends.
Inputs may be any that keep to these rules, and one draw needn't show every extreme that they name: Each row of slot_map is a permutation of 0 to 31.
All inputs are finite; a program needn't handle non-finite values.
Results may differ from the reference program's by a relative error of at most 0.00015.
Values sent between devices are 32-bit elements; how exact they have to be, the bound alone decides.
A program may use at most 64 MiB of HBM per device.

```python
import math
import jax
import jax.numpy as jnp
from jax import lax

K = 120
KEEP = 40
DEG = 3
M = 120
NDEV = 32
BS = 512
NROWS = 524288


def basis_core(key):
    core_key = jax.random.fold_in(key, 11)
    core = jnp.clip(jax.random.normal(core_key, (K, NROWS), jnp.float32), -5.0, 5.0)
    position = jnp.arange(NROWS, dtype=jnp.float32) / NROWS
    block_scale = jnp.exp(jax.random.uniform(jax.random.fold_in(key, 12), (NROWS // BS,), jnp.float32, math.log(0.5), math.log(2.0)))
    jitter = jax.random.uniform(jax.random.fold_in(key, 13), (NROWS,), jnp.float32, 0.7, 1.3)
    row_scale = (1.0 + 2.0 * position) * jnp.repeat(block_scale, BS) * jitter
    return (core, row_scale)


def draw_u_fem(key, part):
    core, row_scale = basis_core(key)
    width_scale = jnp.exp(jax.random.uniform(jax.random.fold_in(key, 21), (K,), jnp.float32, 0.0, math.log(10.0)))
    mixing = jnp.eye(K, dtype=jnp.float32) + 0.25 * jax.random.normal(jax.random.fold_in(key, 22), (K, K), jnp.float32) / math.sqrt(K)
    mixed = jnp.dot(mixing, core, precision=lax.Precision.HIGHEST)
    values = width_scale[:, None] * mixed * row_scale[None, :]
    return jnp.clip(values, -600.0, 600.0).astype(jnp.float32)


def draw_resid_fem(key, part):
    core, row_scale = basis_core(key)
    weights = jax.random.normal(jax.random.fold_in(key, 31), (K,), jnp.float32) / math.sqrt(K)
    noise = jnp.clip(jax.random.normal(jax.random.fold_in(key, 32), (NROWS,), jnp.float32), -5.0, 5.0)
    values = (jnp.dot(weights, core, precision=lax.Precision.HIGHEST) + noise) * row_scale
    return jnp.clip(values, -60.0, 60.0)[None, :].astype(jnp.float32)


def draw_slot_map(key, part):
    row_keys = jax.random.split(jax.random.fold_in(key, 41), NDEV)
    return jax.vmap(lambda one_key: jax.random.permutation(one_key, NDEV))(row_keys).astype(jnp.int32)


def steps_of(own_key, shape, cuts, least, high):
    def one(dim, parts):
        draws = jax.random.uniform(jax.random.fold_in(jax.random.fold_in(own_key, 6), dim), (parts,), jnp.float32, least / len(cuts), high / len(cuts))
        return jnp.repeat(jnp.exp(draws), shape[dim] // parts).reshape((-1,) + (1,) * (len(shape) - dim - 1))

    gain = one(*cuts[0])
    for cut in cuts[1:]:
        gain = gain * one(*cut)
    return gain


def gaussian(rng, extent, spread, limit, cuts=(), kind=jnp.bfloat16):
    result = spread * jax.random.normal(rng, extent, jnp.float32)
    if cuts:
        result = result * steps_of(rng, extent, cuts, -0.22, 0.18)
    return jnp.clip(result, -limit, limit).astype(kind)


def setup_inputs(seed: int = 0) -> dict:
    seeds = jax.random.split(jax.random.key(seed), 6)
    return {
        "u_fem": draw_u_fem(jax.random.fold_in(seeds[5], 71), 0),
        "resid_fem": draw_resid_fem(jax.random.fold_in(seeds[5], 71), 0),
        "slot_map": draw_slot_map(jax.random.fold_in(seeds[5], 71), 0),
        "restart": gaussian(seeds[3], (K, KEEP), K ** -0.5, 0.5, (), jnp.float32),
        "coeff": gaussian(seeds[4], (DEG, K, M), 1.0, 6.0, ((2, 4),), jnp.float32),
    }


def relayout(values, slot_map):
    width = values.shape[0]
    blocks = values.reshape(width, NDEV, NDEV, BS).transpose(0, 2, 1, 3)
    source = jnp.argsort(slot_map, axis=1).astype(jnp.int32)
    moved = jnp.take_along_axis(blocks, source[None, :, :, None], axis=2)
    return moved.reshape(width, NROWS)

def reference(u_fem, resid_fem, slot_map, restart, coeff):
    highest = lax.Precision.HIGHEST
    gram_sum = jnp.einsum('kn,jn->kj', u_fem, u_fem, precision=highest) / NROWS
    inner_prod = jnp.einsum('kn,n->k', u_fem, resid_fem[0], precision=highest)
    chol_lower = jnp.linalg.cholesky(gram_sum)
    factor = lax.linalg.triangular_solve(chol_lower, restart, left_side=True, lower=True, transpose_a=True)
    new_rows = jnp.einsum('kp,kn->pn', factor, u_fem, precision=highest)
    half_solve = lax.linalg.triangular_solve(chol_lower, inner_prod[:, None], left_side=True, lower=True)
    proj_coef = lax.linalg.triangular_solve(chol_lower, half_solve, left_side=True, lower=True, transpose_a=True)[:, 0] / NROWS
    remainder = resid_fem - jnp.einsum('k,kn->n', proj_coef, u_fem, precision=highest)[None, :]
    norm_sum = jnp.sum(remainder * remainder)
    next_row = remainder * lax.rsqrt(norm_sum / NROWS + 1e-06)
    raised = jnp.dot(chol_lower, restart, precision=highest)
    rotated = jnp.einsum('kp,ikm->ipm', raised, coeff, precision=highest)
    new_coeff = rotated * lax.rsqrt(jnp.mean(rotated * rotated) + 1e-06)
    return (relayout(new_rows, slot_map), relayout(next_row, slot_map), new_coeff)
```

```python
import functools

import jax
import jax.numpy as jnp
from jax import lax
from jax.experimental import pallas as pl
from jax.experimental.pallas import tpu as pltpu

HIGHEST = lax.Precision.HIGHEST
MESH = pl.DeviceIdType.MESH
AXES = ("rows", "sub")
LANES = 128
SUBLANES = 8


def greet_all(me, ndev, ns):
    barrier = pltpu.get_barrier_semaphore()

    def greet(o, carry):
        j = (me + o) % ndev
        pl.semaphore_signal(barrier, inc=1, device_id=(j // ns, j % ns), device_id_type=MESH)
        return carry

    lax.fori_loop(1, ndev, greet, 0)
    return barrier


def gram_piece(u_ref, r_ref, col, chunk):
    cols = pl.ds(col, chunk)
    pad = LANES - u_ref.shape[0]
    first = lax.broadcasted_iota(jnp.int32, (pad, chunk), 0) == 0
    tail = jnp.where(first, jnp.broadcast_to(r_ref[:, cols], (pad, chunk)), 0.0)
    x = jnp.concatenate([u_ref[:, cols], tail], axis=0)
    hi = x.astype(jnp.bfloat16)
    lo = (x - hi.astype(jnp.float32)).astype(jnp.bfloat16)
    both = jnp.concatenate([hi, lo], axis=0)
    return lax.dot_general(both, both, (((1,), (1,)), ((), ())), preferred_element_type=jnp.float32)


def factor_panels(sums_ref, restart_ref, work, upper, nrows, panel):
    keep, k = restart_ref.shape
    width = sums_ref.shape[1]
    row = lax.broadcasted_iota(jnp.int32, (width, width), 0)
    lane = lax.broadcasted_iota(jnp.int32, (width, width), 1)
    line = lax.broadcasted_iota(jnp.int32, (1, width), 1)
    work[:, :width] = sums_ref[...] * (1.0 / nrows)
    work[:, width:] = jnp.where(row == lane, 1.0, 0.0)
    upper[...] = jnp.zeros_like(upper)

    def step(i, carry):
        base = i * panel
        rows = [work[pl.ds(base + a, 1), :] for a in range(panel)]
        left = work[:, :width]
        cols = [jnp.sum(jnp.where(lane == base + a, left, 0.0), axis=1, keepdims=True) for a in range(panel)]
        block = {
            (a, b): jnp.sum(jnp.where(line == base + b, rows[a][:, :width], 0.0), axis=1, keepdims=True)
            for a in range(panel) for b in range(a, panel)
        }
        for a in range(panel):
            inverse = 1.0 / block[a, a]
            for b in range(a + 1, panel):
                ratio = block[a, b] * inverse
                rows[b] = rows[b] - ratio * rows[a]
                cols[b] = cols[b] - ratio * cols[a]
                for c in range(b, panel):
                    block[b, c] = block[b, c] - ratio * block[a, c]
            cols[a] = (cols[a], inverse)
            upper[pl.ds(base + a, 1), :] = rows[a] * lax.rsqrt(block[a, a])
        work[...] = work[...] - sum((cols[a][0] * cols[a][1]) * rows[a] for a in range(panel))
        return carry

    lax.fori_loop(0, k // panel, step, 0)
    both = jnp.dot(restart_ref[...], upper[:k, :], precision=HIGHEST, preferred_element_type=jnp.float32)
    half = upper[:, :width].T[k : k + 8, :]
    proj = jnp.dot(half, upper[:, width:], precision=HIGHEST, preferred_element_type=jnp.float32)
    raised = both[:, :k]
    weights = jnp.concatenate([both[:, width:], proj], axis=0)[:, :k]
    return weights, raised


def restart_kernel(ndev, ns, count, nrows, chunk, u_hbm, r_hbm, restart_hbm, coeff_hbm,
                   big, small, coeff_out, u_ref, r_ref, restart_ref, coeff_ref, part, gathered, red, sums, work, upper, weights_ref,
                   send, row_send, turn_send, turn_mid, turn_all, load_sem, own_sem,
                   s1, r1, s2, r2, s3, r3, s4, r4, s5, r5, s6, r6):
    r, s = lax.axis_index("rows"), lax.axis_index("sub")
    me = r * ns + s
    nr = ndev // ns
    keep, k = restart_ref.shape
    bs = send.shape[2]
    deg, mloc, _ = coeff_ref.shape
    pieces = u_ref.shape[1] // chunk

    def remote(src, dst, send_sem, recv_sem, dev):
        return pltpu.make_async_remote_copy(
            src_ref=src, dst_ref=dst, send_sem=send_sem, recv_sem=recv_sem, device_id=dev, device_id_type=MESH)

    def others(action):
        def body(o, carry):
            action((me + o) % ndev)
            return carry
        lax.fori_loop(1, ndev, body, 0)

    load_r = pltpu.make_async_copy(r_hbm, r_ref, load_sem.at[pieces])
    load_r.start()
    load_small = [pltpu.make_async_copy(restart_hbm, restart_ref, own_sem.at[0]),
                  pltpu.make_async_copy(coeff_hbm, coeff_ref, own_sem.at[1])]
    loads = []
    for c in range(pieces):
        cols = pl.ds(c * chunk, chunk)
        loads.append(pltpu.make_async_copy(u_hbm.at[:, cols], u_ref.at[:, cols], load_sem.at[c]))
        loads[-1].start()
    for load in load_small:
        load.start()
    barrier = greet_all(me, ndev, ns)

    load_r.wait()
    full = jnp.zeros((2 * LANES, 2 * LANES), jnp.float32)
    for c in range(pieces):
        loads[c].wait()
        full = full + gram_piece(u_ref, r_ref, c * chunk, chunk)
    cross = full[:LANES, LANES:]
    part[...] = full[:LANES, :LANES] + (cross + cross.T) + full[LANES:, LANES:]
    pl.semaphore_wait(barrier, ndev - 1)

    groups = part.shape[0] // SUBLANES
    middle = ns - 2 * (ns // 4)
    own = r * middle + s - ns // 4
    owning = (s >= ns // 4) & (s < ns // 4 + middle) & (own < groups)

    def owner(g):
        return g // middle, ns // 4 + g % middle

    def group_rows(ref, g):
        return ref.at[pl.ds(pl.multiple_of(g * SUBLANES, SUBLANES), SUBLANES), :]

    def scatter_copy(g, slot):
        return remote(group_rows(part, g), gathered.at[slot], s1.at[g], r1.at[slot], owner(g))

    def gather_copy(j, g):
        return remote(red, group_rows(sums, g), s2.at[j], r2.at[g], (j // ns, j % ns))

    def groups_not_mine(action):
        def body(o, carry):
            g = (r * middle + o) % groups
            @pl.when(jnp.logical_not(owning & (g == own)))
            def _():
                action(g)
            return carry
        lax.fori_loop(0, groups, body, 0)

    groups_not_mine(lambda g: scatter_copy(g, me).start())

    @pl.when(owning)
    def _():
        mine = pl.ds(pl.multiple_of(own * SUBLANES, SUBLANES), SUBLANES)
        others(lambda j: scatter_copy(own, j).wait_recv())
        gathered[me] = part[mine, :]
        total = jnp.sum(gathered[...], axis=0)
        red[...] = total
        sums[mine, :] = total
        others(lambda j: gather_copy(j, own).start())

    groups_not_mine(lambda g: gather_copy(me, g).wait_recv())

    for load in load_small:
        load.wait()
    panel = next(p for p in (4, 2, 1) if k % p == 0)
    weights, raised = factor_panels(sums, restart_ref, work, upper, nrows, panel)
    weights_ref[...] = weights

    def big_copy(j, slot):
        return remote(send.at[j], big.at[slot], s3.at[j], r3.at[slot], (j // ns, j % ns))

    def small_copy(j, slot):
        return remote(row_send.at[j], small.at[slot], s4.at[j], r4.at[slot], (j // ns, j % ns))

    half = ns // 2
    side, pos = s // half, s % half
    across = [(1 - side) * half + (pos + q) % half for q in range(half)]
    beside = [side * half + (pos + q) % half for q in range(half)]
    order = []
    for q in range(half):
        order += [across[q], beside[half - 1 - q]]

    def step(d, acc):
        for t in order:
            j = ((r + d) % nr) * ns + t
            cols = pl.ds(pl.multiple_of(j * bs, bs), bs)
            y = jnp.dot(weights_ref[...], u_ref[:, cols], precision=HIGHEST, preferred_element_type=jnp.float32)
            rest = r_ref[:, cols] - y[keep : keep + 1, :]
            row_send[j, 0:1, :bs] = rest
            acc = acc + rest * rest

            @pl.when(j != me)
            def _():
                send[j] = y[:keep, :]
                big_copy(j, me).start()

            @pl.when(j == me)
            def _():
                big[me] = y[:keep, :]

        return acc

    acc = step(0, jnp.zeros((1, bs), jnp.float32))

    width = turn_send.shape[1]
    turn_send[...] = jnp.zeros_like(turn_send)
    for i in range(deg):
        turned = lax.dot_general(coeff_ref[i], raised, (((1,), (1,)), ((), ())), precision=HIGHEST,
                                 preferred_element_type=jnp.float32)
        turn_send[:mloc, i * keep : (i + 1) * keep] = turned
    share = turn_mid.shape[1]
    my_rows = pl.ds(pl.multiple_of(r * share, share), share)
    for i in range(nr):
        @pl.when(r == i)
        def _():
            turn_mid[s] = turn_send[i * share : (i + 1) * share, :]

    def turn_copy(t, slot):
        return remote(turn_mid.at[s], turn_mid.at[slot], s5.at[t], r5.at[slot], (r, t))

    def spread_copy(p, slot):
        return remote(turn_mid, turn_all.at[slot], s6.at[p], r6.at[slot], (p, s))

    def along(action):
        for o in range(1, ns):
            action((s + o) % ns)

    def plane(action):
        def body(o, carry):
            action((r + o) % nr)
            return carry
        lax.fori_loop(1, nr, body, 0)

    along(lambda t: turn_copy(t, s).start())
    acc = lax.fori_loop(1, nr, step, acc)
    partial = jnp.sum(acc, axis=1, keepdims=True)

    def mark(j, carry):
        row_send[j, 0:1, bs:] = jnp.broadcast_to(partial, (1, LANES))
        return carry

    lax.fori_loop(0, ndev, mark, 0)
    others(lambda j: small_copy(j, me).start())
    small[me] = row_send[me]
    along(lambda t: turn_copy(t, t).wait_recv())
    plane(lambda p: spread_copy(p, r).start())
    turn_all[r] = turn_mid[...]
    plane(lambda p: spread_copy(p, p).wait_recv())
    columns = []
    for t in range(ns):
        columns.append(jnp.concatenate([turn_all[p, t] for p in range(nr)], axis=0)[:mloc, :])
    turned = jnp.concatenate(columns, axis=0).T
    squares = jnp.sum(turned * turned)
    scale = lax.rsqrt(jnp.full((1, 1), squares / count + 1e-06, jnp.float32))
    for i in range(deg):
        coeff_out[i] = turned[i * keep : (i + 1) * keep, :] * scale

    others(lambda j: big_copy(j, j).wait_recv())
    others(lambda j: small_copy(j, j).wait_recv())
    groups_not_mine(lambda g: scatter_copy(g, me).wait_send())

    @pl.when(owning)
    def _():
        others(lambda j: gather_copy(j, own).wait_send())

    others(lambda j: big_copy(j, me).wait_send())
    others(lambda j: small_copy(j, me).wait_send())
    along(lambda t: turn_copy(t, s).wait_send())
    plane(lambda p: spread_copy(p, r).wait_send())


def restart_call(u, r, restart, coeff_t, ndev, ns):
    f32 = jnp.float32
    bs = u.shape[1] // ndev
    nr = ndev // ns
    keep, k = restart.shape
    deg, mloc, _ = coeff_t.shape
    count = deg * keep * mloc * ns
    chunk = min(2048, u.shape[1])
    groups = LANES // SUBLANES
    share = -(-mloc // nr)
    lanes = -(-deg * keep // LANES) * LANES
    vmem = pl.BlockSpec(memory_space=pltpu.VMEM)
    hbm = pl.BlockSpec(memory_space=pltpu.MemorySpace.HBM)
    dma = pltpu.SemaphoreType.DMA
    return pl.pallas_call(
        functools.partial(restart_kernel, ndev, ns, count, u.shape[1] * ndev, chunk),
        out_shape=(
            pltpu.VMEM((ndev, keep, bs), f32),
            pltpu.VMEM((ndev, 1, bs + LANES), f32),
            pltpu.VMEM((deg, keep, ns * mloc), f32),
        ),
        in_specs=[hbm, hbm, hbm, hbm],
        out_specs=(vmem, vmem, vmem),
        scratch_shapes=[
            pltpu.VMEM(u.shape, f32),
            pltpu.VMEM(r.shape, f32),
            pltpu.VMEM(restart.shape, f32),
            pltpu.VMEM(coeff_t.shape, f32),
            pltpu.VMEM((LANES, LANES), f32),
            pltpu.VMEM((ndev, SUBLANES, LANES), f32),
            pltpu.VMEM((SUBLANES, LANES), f32),
            pltpu.VMEM((LANES, LANES), f32),
            pltpu.VMEM((LANES, 2 * LANES), f32),
            pltpu.VMEM((LANES, 2 * LANES), f32),
            pltpu.VMEM((keep + SUBLANES, k), f32),
            pltpu.VMEM((ndev, keep, bs), f32),
            pltpu.VMEM((ndev, 1, bs + LANES), f32),
            pltpu.VMEM((nr * share, lanes), f32),
            pltpu.VMEM((ns, share, lanes), f32),
            pltpu.VMEM((nr, ns, share, lanes), f32),
            dma((u.shape[1] // chunk + 1,)),
            dma((2,)),
            dma((groups,)), dma((ndev,)),
            dma((ndev,)), dma((groups,)),
            dma((ndev,)), dma((ndev,)),
            dma((ndev,)), dma((ndev,)),
            dma((ns,)), dma((ns,)),
            dma((nr,)), dma((nr,)),
        ],
        compiler_params=pltpu.CompilerParams(
            collective_id=0, has_side_effects=True, vmem_limit_bytes=48 * 1024 * 1024),
    )(*[pltpu.with_memory_space_constraint(a, pltpu.MemorySpace.HBM) for a in (u, r, restart, coeff_t)])


def place_kernel(ndev, nrows, slots, big, small, coeff, rows_out, vec_out, coeff_out, out_sem):
    bs = big.shape[2]

    def put(d):
        cols = pl.ds(pl.multiple_of(slots[0, d] * bs, bs), bs)
        return pltpu.make_async_copy(big.at[d], rows_out.at[:, cols], out_sem.at[d])

    def loop(action):
        def body(d, carry):
            action(d)
            return carry
        lax.fori_loop(0, ndev, body, 0)

    loop(lambda d: put(d).start())
    total = jnp.sum(small[:, 0, bs : bs + LANES], axis=0, keepdims=True)[:, :1]
    scale = lax.rsqrt(total / nrows + 1e-06)
    for d in range(ndev):
        cols = pl.ds(pl.multiple_of(slots[0, d] * bs, bs), bs)
        vec_out[:, cols] = small[d, 0:1, :bs] * scale
    coeff_out[...] = coeff[...]
    loop(lambda d: put(d).wait())


def place(slot_row, big, small, coeff, nrows):
    ndev, keep, bs = big.shape
    vmem = pl.BlockSpec(memory_space=pltpu.VMEM)
    hbm = pl.BlockSpec(memory_space=pltpu.MemorySpace.HBM)
    return pl.pallas_call(
        functools.partial(place_kernel, ndev, nrows),
        out_shape=(
            jax.ShapeDtypeStruct((keep, ndev * bs), jnp.float32),
            jax.ShapeDtypeStruct((1, ndev * bs), jnp.float32),
            jax.ShapeDtypeStruct(coeff.shape, jnp.float32),
        ),
        in_specs=[pl.BlockSpec(memory_space=pltpu.SMEM), vmem, vmem, vmem],
        out_specs=(hbm, vmem, vmem),
        scratch_shapes=[pltpu.SemaphoreType.DMA((ndev,))],
        compiler_params=pltpu.CompilerParams(vmem_limit_bytes=32 * 1024 * 1024),
    )(slot_row, big, small, coeff)


def local(u, r, slot_map, restart, coeff):
    ndev = lax.axis_size(AXES)
    ns = lax.axis_size("sub")
    nrows = u.shape[1] * ndev
    big, small, new_coeff = restart_call(u, r, restart.T, coeff.transpose(0, 2, 1), ndev, ns)
    return place(slot_map, big, small, new_coeff, nrows)


def solution(mesh):
    P = jax.sharding.PartitionSpec
    in_specs = (P(None, AXES), P(None, AXES), P(AXES, None), P(), P(None, None, "sub"))
    out_specs = (P(None, AXES), P(None, AXES), P())
    return jax.shard_map(local, mesh=mesh, in_specs=in_specs, out_specs=out_specs, check_vma=False)
```

```python
import functools

import jax
import jax.numpy as jnp
from jax import lax
from jax.experimental import pallas as pl
from jax.experimental.pallas import tpu as pltpu

HIGHEST = lax.Precision.HIGHEST
MESH = pl.DeviceIdType.MESH
AXES = ("rows", "sub")
LANES = 128
SUBLANES = 8
RAW_BLOCKS = 2


def greet_all(me, ndev, ns):
    barrier = pltpu.get_barrier_semaphore()

    def greet(o, carry):
        j = (me + o) % ndev
        pl.semaphore_signal(barrier, inc=1, device_id=(j // ns, j % ns), device_id_type=MESH)
        return carry

    lax.fori_loop(1, ndev, greet, 0)
    return barrier


def gram_piece(u_ref, r_ref, col, chunk):
    cols = pl.ds(col, chunk)
    pad = LANES - u_ref.shape[0]
    first = lax.broadcasted_iota(jnp.int32, (pad, chunk), 0) == 0
    tail = jnp.where(first, jnp.broadcast_to(r_ref[:, cols], (pad, chunk)), 0.0)
    x = jnp.concatenate([u_ref[:, cols], tail], axis=0)
    hi = x.astype(jnp.bfloat16)
    lo = (x - hi.astype(jnp.float32)).astype(jnp.bfloat16)
    dims = (((1,), (1,)), ((), ()))
    return (lax.dot_general(hi, hi, dims, preferred_element_type=jnp.float32),
            lax.dot_general(hi, lo, dims, preferred_element_type=jnp.float32))


def factor_panels(sums_ref, restart_ref, work, upper, nrows, panel):
    keep, k = restart_ref.shape
    width = sums_ref.shape[1]
    row = lax.broadcasted_iota(jnp.int32, (width, width), 0)
    lane = lax.broadcasted_iota(jnp.int32, (width, width), 1)
    line = lax.broadcasted_iota(jnp.int32, (1, width), 1)
    work[:, :width] = sums_ref[...] * (1.0 / nrows)
    work[:, width:] = jnp.where(row == lane, 1.0, 0.0)
    upper[...] = jnp.zeros_like(upper)

    def step(i, carry):
        base = i * panel
        rows = [work[pl.ds(base + a, 1), :] for a in range(panel)]
        left = work[:, :width]
        cols = [jnp.sum(jnp.where(lane == base + a, left, 0.0), axis=1, keepdims=True) for a in range(panel)]
        block = {
            (a, b): jnp.sum(jnp.where(line == base + b, rows[a][:, :width], 0.0), axis=1, keepdims=True)
            for a in range(panel) for b in range(a, panel)
        }
        for a in range(panel):
            inverse = 1.0 / block[a, a]
            for b in range(a + 1, panel):
                ratio = block[a, b] * inverse
                rows[b] = rows[b] - ratio * rows[a]
                cols[b] = cols[b] - ratio * cols[a]
                for c in range(b, panel):
                    block[b, c] = block[b, c] - ratio * block[a, c]
            cols[a] = (cols[a], inverse)
            upper[pl.ds(base + a, 1), :] = rows[a] * lax.rsqrt(block[a, a])
        work[...] = work[...] - sum((cols[a][0] * cols[a][1]) * rows[a] for a in range(panel))
        return carry

    lax.fori_loop(0, k // panel, step, 0)
    both = jnp.dot(restart_ref[...], upper[:k, :], precision=HIGHEST, preferred_element_type=jnp.float32)
    half = upper[:, :width].T[k : k + 8, :]
    proj = jnp.dot(half, upper[:, width:], precision=HIGHEST, preferred_element_type=jnp.float32)
    raised = both[:, :k]
    weights = jnp.concatenate([both[:, width:], proj], axis=0)[:, :k]
    return weights, raised


def restart_kernel(ndev, ns, count, nrows, chunk, raw, u_hbm, r_hbm, restart_hbm, coeff_hbm,
                   big, small, coeff_out, u_ref, r_ref, restart_ref, coeff_ref, part, gathered, mine_ref, other_ref, red, sums, work, upper, weights_ref,
                   send, row_send, turn_send, turn_mid, turn_all, raw_ref, load_sem, own_sem,
                   s1, r1, s2, r2, s3, r3, s4, r4, s5, r5, s6, r6, s7, r7):
    r, s = lax.axis_index("rows"), lax.axis_index("sub")
    me = r * ns + s
    nr = ndev // ns
    keep, k = restart_ref.shape
    bs = send.shape[2]
    deg, mloc, _ = coeff_ref.shape
    pieces = u_ref.shape[1] // chunk

    def remote(src, dst, send_sem, recv_sem, dev):
        return pltpu.make_async_remote_copy(
            src_ref=src, dst_ref=dst, send_sem=send_sem, recv_sem=recv_sem, device_id=dev, device_id_type=MESH)

    def others(action):
        def body(o, carry):
            action((me + o) % ndev)
            return carry
        lax.fori_loop(1, ndev, body, 0)

    load_r = pltpu.make_async_copy(r_hbm, r_ref, load_sem.at[pieces])
    load_r.start()
    load_small = [pltpu.make_async_copy(restart_hbm, restart_ref, own_sem.at[0]),
                  pltpu.make_async_copy(coeff_hbm, coeff_ref, own_sem.at[1])]
    loads = []
    for c in range(pieces):
        cols = pl.ds(c * chunk, chunk)
        loads.append(pltpu.make_async_copy(u_hbm.at[:, cols], u_ref.at[:, cols], load_sem.at[c]))
        loads[-1].start()
    for load in load_small:
        load.start()
    barrier = greet_all(me, ndev, ns)

    load_r.wait()
    main = jnp.zeros((LANES, LANES), jnp.float32)
    cross = jnp.zeros((LANES, LANES), jnp.float32)
    for c in range(pieces):
        loads[c].wait()
        one, two = gram_piece(u_ref, r_ref, c * chunk, chunk)
        main = main + one
        cross = cross + two
    part[...] = main + (cross + cross.T)
    pl.semaphore_wait(barrier, ndev - 1)

    half = ns // 2
    side, pos = s // half, s % half
    here = r * half + pos
    size = red.shape[0]
    groups = part.shape[0] // size
    own = (r // 2) * half + pos
    owning = (r % 2 == 1) & (own < groups)
    opposite = (r, (s + half) % ns)

    def member(m):
        return m // half, side * half + m % half

    def owner(g):
        return 2 * (g // half) + 1, side * half + g % half

    def group_rows(ref, g):
        return ref.at[pl.ds(pl.multiple_of(g * size, size), size), :]

    def scatter_copy(g, slot):
        return remote(group_rows(part, g), gathered.at[slot], s1.at[g], r1.at[slot], owner(g))

    def cross_copy():
        return remote(mine_ref, other_ref, s2.at[nr * half], r2.at[groups], opposite)

    def gather_copy(m, g):
        return remote(red, group_rows(sums, g), s2.at[m], r2.at[g], member(m))

    def groups_not_mine(action):
        def body(o, carry):
            g = (r // 2 * half + o) % groups
            @pl.when(jnp.logical_not(owning & (g == own)))
            def _():
                action(g)
            return carry
        lax.fori_loop(0, groups, body, 0)

    def half_others(action):
        def body(o, carry):
            action((here + o) % (nr * half))
            return carry
        lax.fori_loop(1, nr * half, body, 0)

    groups_not_mine(lambda g: scatter_copy(g, here).start())

    inner = (s == half - 1) | (s == half)
    facing = ns - 1 - s

    def raw_peer(q):
        return (r // 2 * 2 + (r + q) % 2 + q // 2 * 2) % nr

    def raw_source(q):
        return (r // 2 * 2 + (r + q) % 2 - q // 2 * 2 + nr) % nr

    def raw_copies(q):
        t = raw_peer(q)
        copies = []
        for c in range(bs // LANES):
            cols = pl.ds(pl.multiple_of((t * ns + facing) * bs, LANES) + c * LANES, LANES)
            copies.append(remote(u_ref.at[:, cols], raw_ref.at[q, :, pl.ds(c * LANES, LANES)],
                                 s7.at[q, c], r7.at[q, c], (t, facing)))
        return copies

    def raw_start():
        for q in range(raw):
            for copy in raw_copies(q):
                copy.start()

    def is_raw(j, peer):
        hit = j == peer(0) * ns + facing
        for q in range(1, raw):
            hit = hit | (j == peer(q) * ns + facing)
        return inner & hit

    @pl.when(inner & jnp.logical_not(owning))
    def _():
        raw_start()

    @pl.when(owning)
    def _():
        mine = pl.ds(pl.multiple_of(own * size, size), size)
        half_others(lambda m: scatter_copy(own, m).wait_recv())
        gathered[here] = part[mine, :]
        total = jnp.sum(gathered[...], axis=0)
        mine_ref[...] = total
        cross_copy().start()
        cross_copy().wait_recv()
        total = total + other_ref[...]
        red[...] = total
        sums[mine, :] = total
        half_others(lambda m: gather_copy(m, own).start())

    @pl.when(inner & owning)
    def _():
        raw_start()

    groups_not_mine(lambda g: gather_copy(here, g).wait_recv())

    for load in load_small:
        load.wait()
    panel = next(p for p in (4, 2, 1) if k % p == 0)
    weights, raised = factor_panels(sums, restart_ref, work, upper, nrows, panel)
    weights_ref[...] = weights

    def big_copy(j, slot):
        return remote(send.at[j], big.at[slot], s3.at[j], r3.at[slot], (j // ns, j % ns))

    def small_copy(j, slot):
        return remote(row_send.at[j], small.at[slot], s4.at[j], r4.at[slot], (j // ns, j % ns))

    across = [(1 - side) * half + (pos + q) % half for q in range(half)]
    beside = [side * half + (pos + q) % half for q in range(half)]
    order = []
    for q in range(half):
        order += [(across[q], True), (beside[half - 1 - q], False)]

    def project(j, acc):
        cols = pl.ds(pl.multiple_of(j * bs, bs), bs)
        y = jnp.dot(weights_ref[...], u_ref[:, cols], precision=HIGHEST, preferred_element_type=jnp.float32)
        rest = r_ref[:, cols] - y[keep : keep + 1, :]
        row_send[j, 0:1, :bs] = rest
        return y[:keep, :], acc + rest * rest

    def send_block(j, is_across):
        if is_across:
            @pl.when(jnp.logical_not(is_raw(j, raw_peer)))
            def _():
                big_copy(j, me).start()
        else:
            big_copy(j, me).start()

    def step(d, acc):
        for t, is_across in order:
            j = ((r + d) % nr) * ns + t
            send[j], acc = project(j, acc)
            send_block(j, is_across)
        return acc

    def last_step(acc):
        for t, is_across in order[:-1]:
            j = r * ns + t
            send[j], acc = project(j, acc)
            send_block(j, is_across)
        big[me], acc = project(me, acc)
        return acc

    acc = step(1, jnp.zeros((1, bs), jnp.float32))

    width = turn_send.shape[1]
    turn_send[...] = jnp.zeros_like(turn_send)
    for i in range(deg):
        turned = lax.dot_general(coeff_ref[i], raised, (((1,), (1,)), ((), ())), precision=HIGHEST,
                                 preferred_element_type=jnp.float32)
        turn_send[:mloc, i * keep : (i + 1) * keep] = turned
    share = turn_mid.shape[1]
    my_rows = pl.ds(pl.multiple_of(r * share, share), share)
    for i in range(nr):
        @pl.when(r == i)
        def _():
            turn_mid[s] = turn_send[i * share : (i + 1) * share, :]

    def turn_copy(t, slot):
        return remote(turn_mid.at[s], turn_mid.at[slot], s5.at[t], r5.at[slot], (r, t))

    def spread_copy(p, slot):
        return remote(turn_mid, turn_all.at[slot], s6.at[p], r6.at[slot], (p, s))

    def along(action):
        for o in range(1, ns):
            action((s + o) % ns)

    def plane(action):
        def body(o, carry):
            action((r + o) % nr)
            return carry
        lax.fori_loop(1, nr, body, 0)

    along(lambda t: turn_copy(t, s).start())
    acc = lax.fori_loop(2, nr, step, acc)
    acc = last_step(acc)
    partial = jnp.sum(acc, axis=1, keepdims=True)

    def mark(j, carry):
        row_send[j, 0:1, bs:] = jnp.broadcast_to(partial, (1, LANES))
        return carry

    lax.fori_loop(0, ndev, mark, 0)
    others(lambda j: small_copy(j, me).start())
    small[me] = row_send[me]

    @pl.when(inner)
    def _():
        for q in range(raw):
            for copy in raw_copies(q):
                copy.wait_recv()
            y = jnp.dot(weights_ref[:keep, :], raw_ref[q], precision=HIGHEST, preferred_element_type=jnp.float32)
            big[raw_source(q) * ns + facing] = y

    along(lambda t: turn_copy(t, t).wait_recv())
    plane(lambda p: spread_copy(p, r).start())
    turn_all[r] = turn_mid[...]
    plane(lambda p: spread_copy(p, p).wait_recv())
    columns = []
    for t in range(ns):
        columns.append(jnp.concatenate([turn_all[p, t] for p in range(nr)], axis=0)[:mloc, :])
    turned = jnp.concatenate(columns, axis=0).T
    squares = jnp.sum(turned * turned)
    scale = lax.rsqrt(jnp.full((1, 1), squares / count + 1e-06, jnp.float32))
    for i in range(deg):
        coeff_out[i] = turned[i * keep : (i + 1) * keep, :] * scale

    def others_cooked(peer, action):
        def body(j):
            @pl.when(jnp.logical_not(is_raw(j, peer)))
            def _():
                action(j)
        others(body)

    others_cooked(raw_source, lambda j: big_copy(j, j).wait_recv())
    others(lambda j: small_copy(j, j).wait_recv())
    groups_not_mine(lambda g: scatter_copy(g, here).wait_send())

    @pl.when(owning)
    def _():
        cross_copy().wait_send()
        half_others(lambda m: gather_copy(m, own).wait_send())

    @pl.when(inner)
    def _():
        for q in range(raw):
            for copy in raw_copies(q):
                copy.wait_send()

    others_cooked(raw_peer, lambda j: big_copy(j, me).wait_send())
    others(lambda j: small_copy(j, me).wait_send())
    along(lambda t: turn_copy(t, s).wait_send())
    plane(lambda p: spread_copy(p, r).wait_send())


def restart_call(u, r, restart, coeff_t, ndev, ns):
    f32 = jnp.float32
    bs = u.shape[1] // ndev
    nr = ndev // ns
    keep, k = restart.shape
    deg, mloc, _ = coeff_t.shape
    count = deg * keep * mloc * ns
    chunk = min(2048, u.shape[1])
    size = 2 * SUBLANES
    groups = LANES // size
    share = -(-mloc // nr)
    lanes = -(-deg * keep // LANES) * LANES
    vmem = pl.BlockSpec(memory_space=pltpu.VMEM)
    hbm = pl.BlockSpec(memory_space=pltpu.MemorySpace.HBM)
    dma = pltpu.SemaphoreType.DMA
    return pl.pallas_call(
        functools.partial(restart_kernel, ndev, ns, count, u.shape[1] * ndev, chunk, RAW_BLOCKS),
        out_shape=(
            pltpu.VMEM((ndev, keep, bs), f32),
            pltpu.VMEM((ndev, 1, bs + LANES), f32),
            pltpu.VMEM((deg, keep, ns * mloc), f32),
        ),
        in_specs=[hbm, hbm, hbm, hbm],
        out_specs=(vmem, vmem, vmem),
        scratch_shapes=[
            pltpu.VMEM(u.shape, f32),
            pltpu.VMEM(r.shape, f32),
            pltpu.VMEM(restart.shape, f32),
            pltpu.VMEM(coeff_t.shape, f32),
            pltpu.VMEM((LANES, LANES), f32),
            pltpu.VMEM((ndev // 2, size, LANES), f32),
            pltpu.VMEM((size, LANES), f32),
            pltpu.VMEM((size, LANES), f32),
            pltpu.VMEM((size, LANES), f32),
            pltpu.VMEM((LANES, LANES), f32),
            pltpu.VMEM((LANES, 2 * LANES), f32),
            pltpu.VMEM((LANES, 2 * LANES), f32),
            pltpu.VMEM((keep + SUBLANES, k), f32),
            pltpu.VMEM((ndev, keep, bs), f32),
            pltpu.VMEM((ndev, 1, bs + LANES), f32),
            pltpu.VMEM((nr * share, lanes), f32),
            pltpu.VMEM((ns, share, lanes), f32),
            pltpu.VMEM((nr, ns, share, lanes), f32),
            pltpu.VMEM((RAW_BLOCKS, k, bs), f32),
            dma((u.shape[1] // chunk + 1,)),
            dma((2,)),
            dma((groups,)), dma((ndev // 2,)),
            dma((ndev // 2 + 1,)), dma((groups + 1,)),
            dma((ndev,)), dma((ndev,)),
            dma((ndev,)), dma((ndev,)),
            dma((ns,)), dma((ns,)),
            dma((nr,)), dma((nr,)),
            dma((RAW_BLOCKS, bs // LANES)), dma((RAW_BLOCKS, bs // LANES)),
        ],
        compiler_params=pltpu.CompilerParams(
            collective_id=0, has_side_effects=True, vmem_limit_bytes=48 * 1024 * 1024),
    )(*[pltpu.with_memory_space_constraint(a, pltpu.MemorySpace.HBM) for a in (u, r, restart, coeff_t)])


def place_kernel(ndev, nrows, slots, big, small, coeff, rows_out, vec_out, coeff_out, out_sem):
    bs = big.shape[2]

    def put(d):
        cols = pl.ds(pl.multiple_of(slots[0, d] * bs, bs), bs)
        return pltpu.make_async_copy(big.at[d], rows_out.at[:, cols], out_sem.at[d])

    def loop(action):
        def body(d, carry):
            action(d)
            return carry
        lax.fori_loop(0, ndev, body, 0)

    loop(lambda d: put(d).start())
    total = jnp.sum(small[:, 0, bs : bs + LANES], axis=0, keepdims=True)[:, :1]
    scale = lax.rsqrt(total / nrows + 1e-06)
    for d in range(ndev):
        cols = pl.ds(pl.multiple_of(slots[0, d] * bs, bs), bs)
        vec_out[:, cols] = small[d, 0:1, :bs] * scale
    coeff_out[...] = coeff[...]
    loop(lambda d: put(d).wait())


def place(slot_row, big, small, coeff, nrows):
    ndev, keep, bs = big.shape
    vmem = pl.BlockSpec(memory_space=pltpu.VMEM)
    hbm = pl.BlockSpec(memory_space=pltpu.MemorySpace.HBM)
    return pl.pallas_call(
        functools.partial(place_kernel, ndev, nrows),
        out_shape=(
            jax.ShapeDtypeStruct((keep, ndev * bs), jnp.float32),
            jax.ShapeDtypeStruct((1, ndev * bs), jnp.float32),
            jax.ShapeDtypeStruct(coeff.shape, jnp.float32),
        ),
        in_specs=[pl.BlockSpec(memory_space=pltpu.SMEM), vmem, vmem, vmem],
        out_specs=(hbm, vmem, vmem),
        scratch_shapes=[pltpu.SemaphoreType.DMA((ndev,))],
        compiler_params=pltpu.CompilerParams(vmem_limit_bytes=32 * 1024 * 1024),
    )(slot_row, big, small, coeff)


def local(u, r, slot_map, restart, coeff):
    ndev = lax.axis_size(AXES)
    ns = lax.axis_size("sub")
    nrows = u.shape[1] * ndev
    big, small, new_coeff = restart_call(u, r, restart.T, coeff.transpose(0, 2, 1), ndev, ns)
    return place(slot_map, big, small, new_coeff, nrows)


def solution(mesh):
    P = jax.sharding.PartitionSpec
    in_specs = (P(None, AXES), P(None, AXES), P(AXES, None), P(), P(None, None, "sub"))
    out_specs = (P(None, AXES), P(None, AXES), P())
    return jax.shard_map(local, mesh=mesh, in_specs=in_specs, out_specs=out_specs, check_vma=False)
```

```python
import functools

import jax
import jax.numpy as jnp
from jax import lax
from jax.experimental import pallas as pl
from jax.experimental.pallas import tpu as pltpu

HIGHEST = lax.Precision.HIGHEST
MESH = pl.DeviceIdType.MESH
AXES = ("rows", "sub")
LANES = 128
SUBLANES = 8
RAW_BLOCKS = 2


def greet_all(me, ndev, ns):
    barrier = pltpu.get_barrier_semaphore()

    def greet(o, carry):
        j = (me + o) % ndev
        pl.semaphore_signal(barrier, inc=1, device_id=(j // ns, j % ns), device_id_type=MESH)
        return carry

    lax.fori_loop(1, ndev, greet, 0)
    return barrier


def gram_piece(u_ref, r_ref, col, chunk):
    cols = pl.ds(col, chunk)
    pad = LANES - u_ref.shape[0]
    first = lax.broadcasted_iota(jnp.int32, (pad, chunk), 0) == 0
    tail = jnp.where(first, jnp.broadcast_to(r_ref[:, cols], (pad, chunk)), 0.0)
    x = jnp.concatenate([u_ref[:, cols], tail], axis=0)
    hi = x.astype(jnp.bfloat16)
    lo = (x - hi.astype(jnp.float32)).astype(jnp.bfloat16)
    dims = (((1,), (1,)), ((), ()))
    return (lax.dot_general(hi, hi, dims, preferred_element_type=jnp.float32),
            lax.dot_general(hi, lo, dims, preferred_element_type=jnp.float32))


def lane_sum(x, mask):
    return jnp.broadcast_to(jnp.sum(jnp.where(mask, x, 0.0), axis=1, keepdims=True), x.shape)


def eliminate(d, base, lane, sub):
    n = SUBLANES
    cols = [lane_sum(d, lane == base + b) for b in range(n)]
    block = {(a, b): jnp.broadcast_to(cols[b][a : a + 1, :], d.shape) for b in range(n) for a in range(b + 1)}
    panel = (lane >= base) & (lane < base + n)
    rows = [jnp.where(panel, jnp.where(lane == base + a, 1.0, 0.0), jnp.broadcast_to(d[a : a + 1, :], d.shape))
            for a in range(n)]
    ratio, inverse = {}, []
    for a in range(n):
        inverse.append(1.0 / block[a, a])
        for b in range(a + 1, n):
            ratio[a, b] = block[a, b] * inverse[a]
            for c in range(b, n):
                block[b, c] = block[b, c] - ratio[a, b] * block[a, c]
            rows[b] = rows[b] - ratio[a, b] * rows[a]
    back = [None] * n
    for a in range(n - 1, -1, -1):
        back[a] = rows[a] * inverse[a]
        for c in range(a + 1, n):
            back[a] = back[a] - ratio[a, c] * back[c]
    packed, pivots = rows[0], block[0, 0]
    for a in range(1, n):
        packed = jnp.where(sub == a, rows[a], packed)
        pivots = jnp.where(sub == a, block[a, a], pivots)
    own = jnp.zeros_like(d)
    for b in range(n):
        col = block[0, b]
        for a in range(1, b + 1):
            col = jnp.where(sub == a, block[a, b], col)
        own = jnp.where((lane == base + b) & (sub <= b), col, own)
    scale = lax.rsqrt(pivots)
    left = lane < base + n
    return panel, back, jnp.where(left, packed, 0.0) * scale, jnp.where(left, own, packed) * scale


def factor(sums_ref, nrows, k, work, inverse_ref, upper_ref):
    width = work.shape[1]
    lane = lax.broadcasted_iota(jnp.int32, (SUBLANES, width), 1)
    sub = lax.broadcasted_iota(jnp.int32, (SUBLANES, width), 0)
    work[...] = sums_ref[...] * (1.0 / nrows)

    def step(first, i, carry):
        base = i * SUBLANES
        at = pl.ds(pl.multiple_of(base, SUBLANES), SUBLANES)
        panel, back, inverse_ref[at, :], upper_ref[at, :] = eliminate(work[at, :], base, lane, sub)
        for g in range(first, width // SUBLANES):
            w = work[g * SUBLANES : (g + 1) * SUBLANES, :]
            rest = jnp.where(panel, 0.0, w)
            for b in range(SUBLANES):
                rest = rest - lane_sum(w, lane == base + b) * back[b]
            work[g * SUBLANES : (g + 1) * SUBLANES, :] = rest
        return carry

    steps = k // SUBLANES
    mid = (steps + 1) // 2
    lax.fori_loop(0, mid, functools.partial(step, 1), 0)
    lax.fori_loop(mid, steps, functools.partial(step, mid + 1), 0)
    return work[k : k + SUBLANES, :]


def restart_kernel(ndev, ns, count, nrows, chunk, raw, u_hbm, r_hbm, restart_hbm, coeff_hbm,
                   big, small, coeff_out, u_ref, r_ref, restart_ref, coeff_ref, part, gathered, mine_ref, other_ref, red, sums, work, inverse, upper, weights_ref,
                   send, row_send, turn_send, turn_mid, turn_all, raw_ref, load_sem, own_sem,
                   s1, r1, s2, r2, s3, r3, s4, r4, s5, r5, s6, r6, s7, r7):
    r, s = lax.axis_index("rows"), lax.axis_index("sub")
    me = r * ns + s
    nr = ndev // ns
    keep, k = restart_ref.shape
    bs = send.shape[2]
    deg, mloc, _ = coeff_ref.shape
    pieces = u_ref.shape[1] // chunk

    def remote(src, dst, send_sem, recv_sem, dev):
        return pltpu.make_async_remote_copy(
            src_ref=src, dst_ref=dst, send_sem=send_sem, recv_sem=recv_sem, device_id=dev, device_id_type=MESH)

    def others(action):
        def body(o, carry):
            action((me + o) % ndev)
            return carry
        lax.fori_loop(1, ndev, body, 0)

    load_r = pltpu.make_async_copy(r_hbm, r_ref, load_sem.at[pieces])
    load_r.start()
    load_small = [pltpu.make_async_copy(restart_hbm, restart_ref, own_sem.at[0]),
                  pltpu.make_async_copy(coeff_hbm, coeff_ref, own_sem.at[1])]
    loads = []
    for c in range(pieces):
        cols = pl.ds(c * chunk, chunk)
        loads.append(pltpu.make_async_copy(u_hbm.at[:, cols], u_ref.at[:, cols], load_sem.at[c]))
        loads[-1].start()
    for load in load_small:
        load.start()
    barrier = greet_all(me, ndev, ns)

    load_r.wait()
    main = jnp.zeros((LANES, LANES), jnp.float32)
    cross = jnp.zeros((LANES, LANES), jnp.float32)
    for c in range(pieces):
        loads[c].wait()
        one, two = gram_piece(u_ref, r_ref, c * chunk, chunk)
        main = main + one
        cross = cross + two
    part[...] = main + (cross + cross.T)
    pl.semaphore_wait(barrier, ndev - 1)

    half = ns // 2
    side, pos = s // half, s % half
    here = r * half + pos
    size = red.shape[0]
    groups = part.shape[0] // size
    own = (r // 2) * half + pos
    owning = (r % 2 == 1) & (own < groups)
    opposite = (r, (s + half) % ns)

    def member(m):
        return m // half, side * half + m % half

    def owner(g):
        return 2 * (g // half) + 1, side * half + g % half

    def group_rows(ref, g):
        return ref.at[pl.ds(pl.multiple_of(g * size, size), size), :]

    def scatter_copy(g, slot):
        return remote(group_rows(part, g), gathered.at[slot], s1.at[g], r1.at[slot], owner(g))

    def cross_copy():
        return remote(mine_ref, other_ref, s2.at[nr * half], r2.at[groups], opposite)

    def gather_copy(m, g):
        return remote(red, group_rows(sums, g), s2.at[m], r2.at[g], member(m))

    def groups_not_mine(action):
        def body(o, carry):
            g = (r // 2 * half + o) % groups
            @pl.when(jnp.logical_not(owning & (g == own)))
            def _():
                action(g)
            return carry
        lax.fori_loop(0, groups, body, 0)

    def half_others(action):
        def body(o, carry):
            action((here + o) % (nr * half))
            return carry
        lax.fori_loop(1, nr * half, body, 0)

    groups_not_mine(lambda g: scatter_copy(g, here).start())

    inner = (s == half - 1) | (s == half)
    facing = ns - 1 - s

    def raw_peer(q):
        return (r // 2 * 2 + (r + q) % 2 + q // 2 * 2) % nr

    def raw_source(q):
        return (r // 2 * 2 + (r + q) % 2 - q // 2 * 2 + nr) % nr

    def raw_copies(q):
        t = raw_peer(q)
        copies = []
        for c in range(bs // LANES):
            cols = pl.ds(pl.multiple_of((t * ns + facing) * bs, LANES) + c * LANES, LANES)
            copies.append(remote(u_ref.at[:, cols], raw_ref.at[q, :, pl.ds(c * LANES, LANES)],
                                 s7.at[q, c], r7.at[q, c], (t, facing)))
        return copies

    def raw_start():
        for q in range(raw):
            for copy in raw_copies(q):
                copy.start()

    def is_raw(j, peer):
        hit = j == peer(0) * ns + facing
        for q in range(1, raw):
            hit = hit | (j == peer(q) * ns + facing)
        return inner & hit

    @pl.when(inner & jnp.logical_not(owning))
    def _():
        raw_start()

    @pl.when(owning)
    def _():
        mine = pl.ds(pl.multiple_of(own * size, size), size)
        half_others(lambda m: scatter_copy(own, m).wait_recv())
        gathered[here] = part[mine, :]
        total = jnp.sum(gathered[...], axis=0)
        mine_ref[...] = total
        cross_copy().start()
        cross_copy().wait_recv()
        total = total + other_ref[...]
        red[...] = total
        sums[mine, :] = total
        half_others(lambda m: gather_copy(m, own).start())

    @pl.when(inner & owning)
    def _():
        raw_start()

    groups_not_mine(lambda g: gather_copy(here, g).wait_recv())

    for load in load_small:
        load.wait()
    last = factor(sums, nrows, k, work, inverse, upper)
    weights_ref[:keep, :] = jnp.dot(restart_ref[...], inverse[...], precision=HIGHEST,
                                    preferred_element_type=jnp.float32)[:, :k]
    weights_ref[keep:, :] = -last[:, :k]

    def big_copy(j, slot):
        return remote(send.at[j], big.at[slot], s3.at[j], r3.at[slot], (j // ns, j % ns))

    def small_copy(j, slot):
        return remote(row_send.at[j], small.at[slot], s4.at[j], r4.at[slot], (j // ns, j % ns))

    across = [(1 - side) * half + (pos + q) % half for q in range(half)]
    beside = [side * half + (pos + q) % half for q in range(half)]
    order = []
    for q in range(half):
        order += [(across[q], True), (beside[half - 1 - q], False)]

    def project(j, acc):
        cols = pl.ds(pl.multiple_of(j * bs, bs), bs)
        y = jnp.dot(weights_ref[...], u_ref[:, cols], precision=HIGHEST, preferred_element_type=jnp.float32)
        rest = r_ref[:, cols] - y[keep : keep + 1, :]
        row_send[j, 0:1, :bs] = rest
        return y[:keep, :], acc + rest * rest

    def send_block(j, is_across):
        if is_across:
            @pl.when(jnp.logical_not(is_raw(j, raw_peer)))
            def _():
                big_copy(j, me).start()
        else:
            big_copy(j, me).start()

    def step(d, acc):
        for t, is_across in order:
            j = ((r + d) % nr) * ns + t
            send[j], acc = project(j, acc)
            send_block(j, is_across)
        return acc

    def last_step(acc):
        for t, is_across in order[:-1]:
            j = r * ns + t
            send[j], acc = project(j, acc)
            send_block(j, is_across)
        big[me], acc = project(me, acc)
        return acc

    acc = step(1, jnp.zeros((1, bs), jnp.float32))

    raised = jnp.dot(restart_ref[...], upper[...], precision=HIGHEST, preferred_element_type=jnp.float32)[:, :k]
    turn_send[...] = jnp.zeros_like(turn_send)
    for i in range(deg):
        turned = lax.dot_general(coeff_ref[i], raised, (((1,), (1,)), ((), ())), precision=HIGHEST,
                                 preferred_element_type=jnp.float32)
        turn_send[:mloc, i * keep : (i + 1) * keep] = turned
    share = turn_mid.shape[1]
    my_rows = pl.ds(pl.multiple_of(r * share, share), share)
    for i in range(nr):
        @pl.when(r == i)
        def _():
            turn_mid[s] = turn_send[i * share : (i + 1) * share, :]

    def turn_copy(t, slot):
        return remote(turn_mid.at[s], turn_mid.at[slot], s5.at[t], r5.at[slot], (r, t))

    def spread_copy(p, slot):
        return remote(turn_mid, turn_all.at[slot], s6.at[p], r6.at[slot], (p, s))

    def along(action):
        for o in range(1, ns):
            action((s + o) % ns)

    def plane(action):
        def body(o, carry):
            action((r + o) % nr)
            return carry
        lax.fori_loop(1, nr, body, 0)

    along(lambda t: turn_copy(t, s).start())
    acc = lax.fori_loop(2, nr, step, acc)
    acc = last_step(acc)
    partial = jnp.sum(acc, axis=1, keepdims=True)

    def mark(j, carry):
        row_send[j, 0:1, bs:] = jnp.broadcast_to(partial, (1, LANES))
        return carry

    lax.fori_loop(0, ndev, mark, 0)
    others(lambda j: small_copy(j, me).start())
    small[me] = row_send[me]

    @pl.when(inner)
    def _():
        for q in range(raw):
            for copy in raw_copies(q):
                copy.wait_recv()
            y = jnp.dot(weights_ref[:keep, :], raw_ref[q], precision=HIGHEST, preferred_element_type=jnp.float32)
            big[raw_source(q) * ns + facing] = y

    along(lambda t: turn_copy(t, t).wait_recv())
    plane(lambda p: spread_copy(p, r).start())
    turn_all[r] = turn_mid[...]
    plane(lambda p: spread_copy(p, p).wait_recv())
    columns = []
    for t in range(ns):
        columns.append(jnp.concatenate([turn_all[p, t] for p in range(nr)], axis=0)[:mloc, :])
    turned = jnp.concatenate(columns, axis=0).T
    squares = jnp.sum(turned * turned)
    scale = lax.rsqrt(jnp.full((1, 1), squares / count + 1e-06, jnp.float32))
    for i in range(deg):
        coeff_out[i] = turned[i * keep : (i + 1) * keep, :] * scale

    def others_cooked(peer, action):
        def body(j):
            @pl.when(jnp.logical_not(is_raw(j, peer)))
            def _():
                action(j)
        others(body)

    others_cooked(raw_source, lambda j: big_copy(j, j).wait_recv())
    others(lambda j: small_copy(j, j).wait_recv())
    groups_not_mine(lambda g: scatter_copy(g, here).wait_send())

    @pl.when(owning)
    def _():
        cross_copy().wait_send()
        half_others(lambda m: gather_copy(m, own).wait_send())

    @pl.when(inner)
    def _():
        for q in range(raw):
            for copy in raw_copies(q):
                copy.wait_send()

    others_cooked(raw_peer, lambda j: big_copy(j, me).wait_send())
    others(lambda j: small_copy(j, me).wait_send())
    along(lambda t: turn_copy(t, s).wait_send())
    plane(lambda p: spread_copy(p, r).wait_send())


def restart_call(u, r, restart, coeff_t, ndev, ns):
    f32 = jnp.float32
    bs = u.shape[1] // ndev
    nr = ndev // ns
    keep, k = restart.shape
    deg, mloc, _ = coeff_t.shape
    count = deg * keep * mloc * ns
    chunk = min(2048, u.shape[1])
    size = 2 * SUBLANES
    groups = LANES // size
    share = -(-mloc // nr)
    lanes = -(-deg * keep // LANES) * LANES
    vmem = pl.BlockSpec(memory_space=pltpu.VMEM)
    hbm = pl.BlockSpec(memory_space=pltpu.MemorySpace.HBM)
    dma = pltpu.SemaphoreType.DMA
    return pl.pallas_call(
        functools.partial(restart_kernel, ndev, ns, count, u.shape[1] * ndev, chunk, RAW_BLOCKS),
        out_shape=(
            pltpu.VMEM((ndev, keep, bs), f32),
            pltpu.VMEM((ndev, 1, bs + LANES), f32),
            pltpu.VMEM((deg, keep, ns * mloc), f32),
        ),
        in_specs=[hbm, hbm, hbm, hbm],
        out_specs=(vmem, vmem, vmem),
        scratch_shapes=[
            pltpu.VMEM(u.shape, f32),
            pltpu.VMEM(r.shape, f32),
            pltpu.VMEM(restart.shape, f32),
            pltpu.VMEM(coeff_t.shape, f32),
            pltpu.VMEM((LANES, LANES), f32),
            pltpu.VMEM((ndev // 2, size, LANES), f32),
            pltpu.VMEM((size, LANES), f32),
            pltpu.VMEM((size, LANES), f32),
            pltpu.VMEM((size, LANES), f32),
            pltpu.VMEM((LANES, LANES), f32),
            pltpu.VMEM((LANES, LANES), f32),
            pltpu.VMEM((k, LANES), f32),
            pltpu.VMEM((k, LANES), f32),
            pltpu.VMEM((keep + SUBLANES, k), f32),
            pltpu.VMEM((ndev, keep, bs), f32),
            pltpu.VMEM((ndev, 1, bs + LANES), f32),
            pltpu.VMEM((nr * share, lanes), f32),
            pltpu.VMEM((ns, share, lanes), f32),
            pltpu.VMEM((nr, ns, share, lanes), f32),
            pltpu.VMEM((RAW_BLOCKS, k, bs), f32),
            dma((u.shape[1] // chunk + 1,)),
            dma((2,)),
            dma((groups,)), dma((ndev // 2,)),
            dma((ndev // 2 + 1,)), dma((groups + 1,)),
            dma((ndev,)), dma((ndev,)),
            dma((ndev,)), dma((ndev,)),
            dma((ns,)), dma((ns,)),
            dma((nr,)), dma((nr,)),
            dma((RAW_BLOCKS, bs // LANES)), dma((RAW_BLOCKS, bs // LANES)),
        ],
        compiler_params=pltpu.CompilerParams(
            collective_id=0, has_side_effects=True, vmem_limit_bytes=48 * 1024 * 1024),
    )(*[pltpu.with_memory_space_constraint(a, pltpu.MemorySpace.HBM) for a in (u, r, restart, coeff_t)])


def place_kernel(ndev, nrows, slots, big, small, coeff, rows_out, vec_out, coeff_out, out_sem):
    bs = big.shape[2]

    def put(d):
        cols = pl.ds(pl.multiple_of(slots[0, d] * bs, bs), bs)
        return pltpu.make_async_copy(big.at[d], rows_out.at[:, cols], out_sem.at[d])

    def loop(action):
        def body(d, carry):
            action(d)
            return carry
        lax.fori_loop(0, ndev, body, 0)

    loop(lambda d: put(d).start())
    total = jnp.sum(small[:, 0, bs : bs + LANES], axis=0, keepdims=True)[:, :1]
    scale = lax.rsqrt(total / nrows + 1e-06)
    for d in range(ndev):
        cols = pl.ds(pl.multiple_of(slots[0, d] * bs, bs), bs)
        vec_out[:, cols] = small[d, 0:1, :bs] * scale
    coeff_out[...] = coeff[...]
    loop(lambda d: put(d).wait())


def place(slot_row, big, small, coeff, nrows):
    ndev, keep, bs = big.shape
    vmem = pl.BlockSpec(memory_space=pltpu.VMEM)
    hbm = pl.BlockSpec(memory_space=pltpu.MemorySpace.HBM)
    return pl.pallas_call(
        functools.partial(place_kernel, ndev, nrows),
        out_shape=(
            jax.ShapeDtypeStruct((keep, ndev * bs), jnp.float32),
            jax.ShapeDtypeStruct((1, ndev * bs), jnp.float32),
            jax.ShapeDtypeStruct(coeff.shape, jnp.float32),
        ),
        in_specs=[pl.BlockSpec(memory_space=pltpu.SMEM), vmem, vmem, vmem],
        out_specs=(hbm, vmem, vmem),
        scratch_shapes=[pltpu.SemaphoreType.DMA((ndev,))],
        compiler_params=pltpu.CompilerParams(vmem_limit_bytes=32 * 1024 * 1024),
    )(slot_row, big, small, coeff)


def local(u, r, slot_map, restart, coeff):
    ndev = lax.axis_size(AXES)
    ns = lax.axis_size("sub")
    nrows = u.shape[1] * ndev
    big, small, new_coeff = restart_call(u, r, restart.T, coeff.transpose(0, 2, 1), ndev, ns)
    return place(slot_map, big, small, new_coeff, nrows)


def solution(mesh):
    P = jax.sharding.PartitionSpec
    in_specs = (P(None, AXES), P(None, AXES), P(AXES, None), P(), P(None, None, "sub"))
    out_specs = (P(None, AXES), P(None, AXES), P())
    return jax.shard_map(local, mesh=mesh, in_specs=in_specs, out_specs=out_specs, check_vma=False)
```

```python
import functools

import jax
import jax.numpy as jnp
from jax import lax
from jax.experimental import pallas as pl
from jax.experimental.pallas import tpu as pltpu

HIGHEST = lax.Precision.HIGHEST
MESH = pl.DeviceIdType.MESH
AXES = ("rows", "sub")
LANES = 128
SUBLANES = 8
RAW_BLOCKS = (2, 2)
HELD_FROM = 4


def greet_all(me, ndev, ns):
    barrier = pltpu.get_barrier_semaphore()

    def greet(o, carry):
        j = (me + o) % ndev
        pl.semaphore_signal(barrier, inc=1, device_id=(j // ns, j % ns), device_id_type=MESH)
        return carry

    lax.fori_loop(1, ndev, greet, 0)
    return barrier


def gram_piece(u_ref, r_ref, col, chunk):
    cols = pl.ds(col, chunk)
    pad = LANES - u_ref.shape[0]
    first = lax.broadcasted_iota(jnp.int32, (pad, chunk), 0) == 0
    tail = jnp.where(first, jnp.broadcast_to(r_ref[:, cols], (pad, chunk)), 0.0)
    x = jnp.concatenate([u_ref[:, cols], tail], axis=0)
    hi = x.astype(jnp.bfloat16)
    lo = (x - hi.astype(jnp.float32)).astype(jnp.bfloat16)
    dims = (((1,), (1,)), ((), ()))
    return (lax.dot_general(hi, hi, dims, preferred_element_type=jnp.float32),
            lax.dot_general(hi, lo, dims, preferred_element_type=jnp.float32))


def lane_sum(x, mask):
    return jnp.broadcast_to(jnp.sum(jnp.where(mask, x, 0.0), axis=1, keepdims=True), x.shape)


def eliminate(d, base, lane, sub):
    n = SUBLANES
    cols = [lane_sum(d, lane == base + b) for b in range(n)]
    block = {(a, b): jnp.broadcast_to(cols[b][a : a + 1, :], d.shape) for b in range(n) for a in range(b + 1)}
    panel = (lane >= base) & (lane < base + n)
    rows = [jnp.where(panel, jnp.where(lane == base + a, 1.0, 0.0), jnp.broadcast_to(d[a : a + 1, :], d.shape))
            for a in range(n)]
    ratio, inverse = {}, []
    for a in range(n):
        inverse.append(1.0 / block[a, a])
        for b in range(a + 1, n):
            ratio[a, b] = block[a, b] * inverse[a]
            for c in range(b, n):
                block[b, c] = block[b, c] - ratio[a, b] * block[a, c]
            rows[b] = rows[b] - ratio[a, b] * rows[a]
    back = [None] * n
    for a in range(n - 1, -1, -1):
        back[a] = rows[a] * inverse[a]
        for c in range(a + 1, n):
            back[a] = back[a] - ratio[a, c] * back[c]
    packed, pivots = rows[0], block[0, 0]
    for a in range(1, n):
        packed = jnp.where(sub == a, rows[a], packed)
        pivots = jnp.where(sub == a, block[a, a], pivots)
    own = jnp.zeros_like(d)
    for b in range(n):
        col = block[0, b]
        for a in range(1, b + 1):
            col = jnp.where(sub == a, block[a, b], col)
        own = jnp.where((lane == base + b) & (sub <= b), col, own)
    scale = lax.rsqrt(pivots)
    left = lane < base + n
    return panel, back, jnp.where(left, packed, 0.0) * scale, jnp.where(left, own, packed) * scale


def factor(sums_ref, nrows, k, work, inverse_ref, upper_ref):
    width = work.shape[1]
    lane = lax.broadcasted_iota(jnp.int32, (SUBLANES, width), 1)
    sub = lax.broadcasted_iota(jnp.int32, (SUBLANES, width), 0)
    work[...] = sums_ref[...] * (1.0 / nrows)

    def step(first, i, carry):
        base = i * SUBLANES
        at = pl.ds(pl.multiple_of(base, SUBLANES), SUBLANES)
        panel, back, inverse_ref[at, :], upper_ref[at, :] = eliminate(work[at, :], base, lane, sub)
        for g in range(first, width // SUBLANES):
            w = work[g * SUBLANES : (g + 1) * SUBLANES, :]
            rest = jnp.where(panel, 0.0, w)
            for b in range(SUBLANES):
                rest = rest - lane_sum(w, lane == base + b) * back[b]
            work[g * SUBLANES : (g + 1) * SUBLANES, :] = rest
        return carry

    steps = k // SUBLANES
    mid = (steps + 1) // 2
    lax.fori_loop(0, mid, functools.partial(step, 1), 0)
    lax.fori_loop(mid, steps, functools.partial(step, mid + 1), 0)
    return work[k : k + SUBLANES, :]


def restart_kernel(ndev, ns, count, nrows, chunk, raw, u_hbm, r_hbm, restart_hbm, coeff_hbm,
                   big, small, coeff_out, u_ref, r_ref, restart_ref, coeff_ref, part, gathered, mine_ref, other_ref, red, sums, work, inverse, upper, weights_ref,
                   send, row_send, turn_send, turn_mid, turn_all, raw_ref, load_sem, own_sem,
                   s1, r1, s2, r2, s3, r3, s4, r4, s5, r5, s6, r6, s7, r7):
    r, s = lax.axis_index("rows"), lax.axis_index("sub")
    me = r * ns + s
    nr = ndev // ns
    keep, k = restart_ref.shape
    bs = send.shape[2]
    deg, mloc, _ = coeff_ref.shape
    pieces = u_ref.shape[1] // chunk

    def remote(src, dst, send_sem, recv_sem, dev):
        return pltpu.make_async_remote_copy(
            src_ref=src, dst_ref=dst, send_sem=send_sem, recv_sem=recv_sem, device_id=dev, device_id_type=MESH)

    def others(action):
        def body(o, carry):
            action((me + o) % ndev)
            return carry
        lax.fori_loop(1, ndev, body, 0)

    load_r = pltpu.make_async_copy(r_hbm, r_ref, load_sem.at[pieces])
    load_r.start()
    load_small = [pltpu.make_async_copy(restart_hbm, restart_ref, own_sem.at[0]),
                  pltpu.make_async_copy(coeff_hbm, coeff_ref, own_sem.at[1])]
    loads = []
    for c in range(pieces):
        cols = pl.ds(c * chunk, chunk)
        loads.append(pltpu.make_async_copy(u_hbm.at[:, cols], u_ref.at[:, cols], load_sem.at[c]))
        loads[-1].start()
    for load in load_small:
        load.start()
    barrier = greet_all(me, ndev, ns)

    load_r.wait()
    main = jnp.zeros((LANES, LANES), jnp.float32)
    cross = jnp.zeros((LANES, LANES), jnp.float32)
    for c in range(pieces):
        loads[c].wait()
        one, two = gram_piece(u_ref, r_ref, c * chunk, chunk)
        main = main + one
        cross = cross + two
    part[...] = main + (cross + cross.T)
    pl.semaphore_wait(barrier, ndev - 1)

    half = ns // 2
    side, pos = s // half, s % half
    here = r * half + pos
    size = red.shape[0]
    groups = part.shape[0] // size
    own = (r // 2) * half + pos
    owning = (r % 2 == 1) & (own < groups)
    opposite = (r, (s + half) % ns)

    def member(m):
        return m // half, side * half + m % half

    def owner(g):
        return 2 * (g // half) + 1, side * half + g % half

    def group_rows(ref, g):
        return ref.at[pl.ds(pl.multiple_of(g * size, size), size), :]

    def scatter_copy(g, slot):
        return remote(group_rows(part, g), gathered.at[slot], s1.at[g], r1.at[slot], owner(g))

    def cross_copy():
        return remote(mine_ref, other_ref, s2.at[nr * half], r2.at[groups], opposite)

    def gather_copy(m, g):
        return remote(red, group_rows(sums, g), s2.at[m], r2.at[g], member(m))

    def groups_not_mine(action):
        def body(o, carry):
            g = (r // 2 * half + o) % groups
            @pl.when(jnp.logical_not(owning & (g == own)))
            def _():
                action(g)
            return carry
        lax.fori_loop(0, groups, body, 0)

    def half_others(action):
        def body(o, carry):
            action((here + o) % (nr * half))
            return carry
        lax.fori_loop(1, nr * half, body, 0)

    groups_not_mine(lambda g: scatter_copy(g, here).start())

    inner = (s == half - 1) | (s == half)
    facing = ns - 1 - s

    def raw_peer(q):
        return (r // 2 * 2 + (r + q) % 2 + q // 2 * 2) % nr

    def raw_source(q):
        return (r // 2 * 2 + (r + q) % 2 - q // 2 * 2 + nr) % nr

    def raw_copy(q):
        t = raw_peer(q)
        cols = pl.ds(pl.multiple_of((t * ns + facing) * bs, LANES), bs)
        return remote(u_ref.at[:, cols], raw_ref.at[q], s7.at[q], r7.at[q], (t, facing))

    def for_raw(sender, action):
        for q in range(raw[0]):
            if q < raw[1]:
                action(q)
            else:
                @pl.when(sender(q) % 2 == 0)
                def _():
                    action(q)

    def raw_start():
        for_raw(lambda q: r, lambda q: raw_copy(q).start())

    def is_raw(j, peer, sender):
        hit = j < 0
        for q in range(raw[0]):
            one = j == peer(q) * ns + facing
            hit = hit | (one if q < raw[1] else one & (sender(q) % 2 == 0))
        return inner & hit

    def sent_raw(j):
        return is_raw(j, raw_peer, lambda q: r)

    def came_raw(j):
        return is_raw(j, raw_source, raw_source)

    @pl.when(inner & jnp.logical_not(owning))
    def _():
        raw_start()

    @pl.when(owning)
    def _():
        mine = pl.ds(pl.multiple_of(own * size, size), size)
        half_others(lambda m: scatter_copy(own, m).wait_recv())
        gathered[here] = part[mine, :]
        total = jnp.sum(gathered[...], axis=0)
        mine_ref[...] = total
        cross_copy().start()
        cross_copy().wait_recv()
        total = total + other_ref[...]
        red[...] = total
        sums[mine, :] = total
        half_others(lambda m: gather_copy(m, own).start())

    @pl.when(inner & owning)
    def _():
        raw_start()

    groups_not_mine(lambda g: gather_copy(here, g).wait_recv())

    for load in load_small:
        load.wait()
    last = factor(sums, nrows, k, work, inverse, upper)
    weights_ref[:keep, :] = jnp.dot(restart_ref[...], inverse[...], precision=HIGHEST,
                                    preferred_element_type=jnp.float32)[:, :k]
    weights_ref[keep:, :] = -last[:, :k]

    def big_copy(j, slot):
        return remote(send.at[j], big.at[slot], s3.at[j], r3.at[slot], (j // ns, j % ns))

    def small_copy(j, slot):
        return remote(row_send.at[j], small.at[slot], s4.at[j], r4.at[slot], (j // ns, j % ns))

    across = [(1 - side) * half + (pos + q) % half for q in range(half)]
    beside = [side * half + (pos + q) % half for q in range(half)]
    order = []
    for q in range(half):
        order += [(across[q], True), (beside[half - 1 - q], False)]

    def project(j, acc):
        cols = pl.ds(pl.multiple_of(j * bs, bs), bs)
        y = jnp.dot(weights_ref[...], u_ref[:, cols], precision=HIGHEST, preferred_element_type=jnp.float32)
        rest = r_ref[:, cols] - y[keep : keep + 1, :]
        row_send[j, 0:1, :bs] = rest
        return y[:keep, :], acc + rest * rest

    def send_block(j, is_across):
        if is_across:
            @pl.when(jnp.logical_not(sent_raw(j)))
            def _():
                big_copy(j, me).start()
        else:
            big_copy(j, me).start()

    def step(d, acc):
        for t, is_across in order:
            j = ((r + d) % nr) * ns + t
            send[j], acc = project(j, acc)
            send_block(j, is_across)
        return acc

    def hold(d, acc):
        for t, _ in order:
            j = ((r + d) % nr) * ns + t
            send[j], acc = project(j, acc)
        return acc

    def release(d, carry):
        for t, is_across in order:
            send_block(((r + d) % nr) * ns + t, is_across)
        return carry

    acc = step(1, jnp.zeros((1, bs), jnp.float32))

    raised = jnp.dot(restart_ref[...], upper[...], precision=HIGHEST, preferred_element_type=jnp.float32)[:, :k]
    turn_send[...] = jnp.zeros_like(turn_send)
    for i in range(deg):
        turned = lax.dot_general(coeff_ref[i], raised, (((1,), (1,)), ((), ())), precision=HIGHEST,
                                 preferred_element_type=jnp.float32)
        turn_send[:mloc, i * keep : (i + 1) * keep] = turned
    share = turn_mid.shape[1]
    my_rows = pl.ds(pl.multiple_of(r * share, share), share)
    for i in range(nr):
        @pl.when(r == i)
        def _():
            turn_mid[s] = turn_send[i * share : (i + 1) * share, :]

    def turn_copy(t, slot):
        return remote(turn_mid.at[s], turn_mid.at[slot], s5.at[t], r5.at[slot], (r, t))

    def spread_copy(p, slot):
        return remote(turn_mid, turn_all.at[slot], s6.at[p], r6.at[slot], (p, s))

    def along(action):
        for o in range(1, ns):
            action((s + o) % ns)

    def plane(action):
        def body(o, carry):
            action((r + o) % nr)
            return carry
        lax.fori_loop(1, nr, body, 0)

    along(lambda t: turn_copy(t, s).start())
    held = min(nr, HELD_FROM)
    acc = lax.fori_loop(2, held, step, acc)
    acc = lax.fori_loop(held, nr, hold, acc)
    for t, _ in order[:-1]:
        j = r * ns + t
        send[j], acc = project(j, acc)
    big[me], acc = project(me, acc)
    partial = jnp.sum(acc, axis=1, keepdims=True)

    def mark(j, carry):
        row_send[j, 0:1, bs:] = jnp.broadcast_to(partial, (1, LANES))
        return carry

    lax.fori_loop(0, ndev, mark, 0)
    others(lambda j: small_copy(j, me).start())
    lax.fori_loop(held, nr, release, 0)
    for t, is_across in order[:-1]:
        send_block(r * ns + t, is_across)
    small[me] = row_send[me]

    @pl.when(inner)
    def _():
        def finish(q):
            raw_copy(q).wait_recv()
            y = jnp.dot(weights_ref[:keep, :], raw_ref[q], precision=HIGHEST, preferred_element_type=jnp.float32)
            big[raw_source(q) * ns + facing] = y
        for_raw(raw_source, finish)

    along(lambda t: turn_copy(t, t).wait_recv())
    plane(lambda p: spread_copy(p, r).start())
    turn_all[r] = turn_mid[...]
    plane(lambda p: spread_copy(p, p).wait_recv())
    columns = []
    for t in range(ns):
        columns.append(jnp.concatenate([turn_all[p, t] for p in range(nr)], axis=0)[:mloc, :])
    turned = jnp.concatenate(columns, axis=0).T
    squares = jnp.sum(turned * turned)
    scale = lax.rsqrt(jnp.full((1, 1), squares / count + 1e-06, jnp.float32))
    for i in range(deg):
        coeff_out[i] = turned[i * keep : (i + 1) * keep, :] * scale

    def others_cooked(skip, action):
        def body(j):
            @pl.when(jnp.logical_not(skip(j)))
            def _():
                action(j)
        others(body)

    others_cooked(came_raw, lambda j: big_copy(j, j).wait_recv())
    others(lambda j: small_copy(j, j).wait_recv())
    groups_not_mine(lambda g: scatter_copy(g, here).wait_send())

    @pl.when(owning)
    def _():
        cross_copy().wait_send()
        half_others(lambda m: gather_copy(m, own).wait_send())

    @pl.when(inner)
    def _():
        for_raw(lambda q: r, lambda q: raw_copy(q).wait_send())

    others_cooked(sent_raw, lambda j: big_copy(j, me).wait_send())
    others(lambda j: small_copy(j, me).wait_send())
    along(lambda t: turn_copy(t, s).wait_send())
    plane(lambda p: spread_copy(p, r).wait_send())


def restart_call(u, r, restart, coeff_t, ndev, ns):
    f32 = jnp.float32
    bs = u.shape[1] // ndev
    nr = ndev // ns
    keep, k = restart.shape
    deg, mloc, _ = coeff_t.shape
    count = deg * keep * mloc * ns
    chunk = min(2048, u.shape[1])
    size = 2 * SUBLANES
    groups = LANES // size
    share = -(-mloc // nr)
    lanes = -(-deg * keep // LANES) * LANES
    vmem = pl.BlockSpec(memory_space=pltpu.VMEM)
    hbm = pl.BlockSpec(memory_space=pltpu.MemorySpace.HBM)
    dma = pltpu.SemaphoreType.DMA
    return pl.pallas_call(
        functools.partial(restart_kernel, ndev, ns, count, u.shape[1] * ndev, chunk, RAW_BLOCKS),
        out_shape=(
            pltpu.VMEM((ndev, keep, bs), f32),
            pltpu.VMEM((ndev, 1, bs + LANES), f32),
            pltpu.VMEM((deg, keep, ns * mloc), f32),
        ),
        in_specs=[hbm, hbm, hbm, hbm],
        out_specs=(vmem, vmem, vmem),
        scratch_shapes=[
            pltpu.VMEM(u.shape, f32),
            pltpu.VMEM(r.shape, f32),
            pltpu.VMEM(restart.shape, f32),
            pltpu.VMEM(coeff_t.shape, f32),
            pltpu.VMEM((LANES, LANES), f32),
            pltpu.VMEM((ndev // 2, size, LANES), f32),
            pltpu.VMEM((size, LANES), f32),
            pltpu.VMEM((size, LANES), f32),
            pltpu.VMEM((size, LANES), f32),
            pltpu.VMEM((LANES, LANES), f32),
            pltpu.VMEM((LANES, LANES), f32),
            pltpu.VMEM((k, LANES), f32),
            pltpu.VMEM((k, LANES), f32),
            pltpu.VMEM((keep + SUBLANES, k), f32),
            pltpu.VMEM((ndev, keep, bs), f32),
            pltpu.VMEM((ndev, 1, bs + LANES), f32),
            pltpu.VMEM((nr * share, lanes), f32),
            pltpu.VMEM((ns, share, lanes), f32),
            pltpu.VMEM((nr, ns, share, lanes), f32),
            pltpu.VMEM((RAW_BLOCKS[0], k, bs), f32),
            dma((u.shape[1] // chunk + 1,)),
            dma((2,)),
            dma((groups,)), dma((ndev // 2,)),
            dma((ndev // 2 + 1,)), dma((groups + 1,)),
            dma((ndev,)), dma((ndev,)),
            dma((ndev,)), dma((ndev,)),
            dma((ns,)), dma((ns,)),
            dma((nr,)), dma((nr,)),
            dma((RAW_BLOCKS[0],)), dma((RAW_BLOCKS[0],)),
        ],
        compiler_params=pltpu.CompilerParams(
            collective_id=0, has_side_effects=True, vmem_limit_bytes=48 * 1024 * 1024),
    )(*[pltpu.with_memory_space_constraint(a, pltpu.MemorySpace.HBM) for a in (u, r, restart, coeff_t)])


def place_kernel(ndev, nrows, slots, big, small, coeff, rows_out, vec_out, coeff_out, vec, out_sem, side_sem):
    bs = big.shape[2]

    def put(d):
        cols = pl.ds(pl.multiple_of(slots[0, d] * bs, bs), bs)
        return pltpu.make_async_copy(big.at[d], rows_out.at[:, cols], out_sem.at[d])

    def loop(action):
        def body(d, carry):
            action(d)
            return carry
        lax.fori_loop(0, ndev, body, 0)

    loop(lambda d: put(d).start())
    put_coeff = pltpu.make_async_copy(coeff, coeff_out, side_sem.at[0])
    put_coeff.start()
    total = jnp.sum(small[:, 0, bs : bs + LANES], axis=0, keepdims=True)[:, :1]
    scale = lax.rsqrt(total / nrows + 1e-06)
    for d in range(ndev):
        cols = pl.ds(pl.multiple_of(slots[0, d] * bs, bs), bs)
        vec[:, cols] = small[d, 0:1, :bs] * scale
    put_vec = pltpu.make_async_copy(vec, vec_out, side_sem.at[1])
    put_vec.start()
    loop(lambda d: put(d).wait())
    put_coeff.wait()
    put_vec.wait()


def place(slot_row, big, small, coeff, nrows):
    ndev, keep, bs = big.shape
    vmem = pl.BlockSpec(memory_space=pltpu.VMEM)
    hbm = pl.BlockSpec(memory_space=pltpu.MemorySpace.HBM)
    return pl.pallas_call(
        functools.partial(place_kernel, ndev, nrows),
        out_shape=(
            jax.ShapeDtypeStruct((keep, ndev * bs), jnp.float32),
            jax.ShapeDtypeStruct((1, ndev * bs), jnp.float32),
            jax.ShapeDtypeStruct(coeff.shape, jnp.float32),
        ),
        in_specs=[pl.BlockSpec(memory_space=pltpu.SMEM), vmem, vmem, vmem],
        out_specs=(hbm, hbm, hbm),
        scratch_shapes=[pltpu.VMEM((1, ndev * bs), jnp.float32), pltpu.SemaphoreType.DMA((ndev,)),
                        pltpu.SemaphoreType.DMA((2,))],
        compiler_params=pltpu.CompilerParams(vmem_limit_bytes=32 * 1024 * 1024),
    )(slot_row, big, small, coeff)


def local(u, r, slot_map, restart, coeff):
    ndev = lax.axis_size(AXES)
    ns = lax.axis_size("sub")
    nrows = u.shape[1] * ndev
    big, small, new_coeff = restart_call(u, r, restart.T, coeff.transpose(0, 2, 1), ndev, ns)
    return place(slot_map, big, small, new_coeff, nrows)


def solution(mesh):
    P = jax.sharding.PartitionSpec
    in_specs = (P(None, AXES), P(None, AXES), P(AXES, None), P(), P(None, None, "sub"))
    out_specs = (P(None, AXES), P(None, AXES), P())
    return jax.shard_map(local, mesh=mesh, in_specs=in_specs, out_specs=out_specs, check_vma=False)
```

```python
import functools

import jax
import jax.numpy as jnp
from jax import lax
from jax.experimental import pallas as pl
from jax.experimental.pallas import tpu as pltpu

HIGHEST = lax.Precision.HIGHEST
MESH = pl.DeviceIdType.MESH
AXES = ("rows", "sub")
LANES = 128
SUBLANES = 8
RAW_BLOCKS = (3, 2)
RAW_AFTER = 5
HELD_FROM = 4


def greet_all(me, ndev, ns):
    barrier = pltpu.get_barrier_semaphore()

    def greet(o, carry):
        j = (me + o) % ndev
        pl.semaphore_signal(barrier, inc=1, device_id=(j // ns, j % ns), device_id_type=MESH)
        return carry

    lax.fori_loop(1, ndev, greet, 0)
    return barrier


def gram_piece(u_ref, r_ref, col, chunk):
    cols = pl.ds(col, chunk)
    pad = LANES - u_ref.shape[0]
    first = lax.broadcasted_iota(jnp.int32, (pad, chunk), 0) == 0
    tail = jnp.where(first, jnp.broadcast_to(r_ref[:, cols], (pad, chunk)), 0.0)
    x = jnp.concatenate([u_ref[:, cols], tail], axis=0)
    hi = x.astype(jnp.bfloat16)
    lo = (x - hi.astype(jnp.float32)).astype(jnp.bfloat16)
    dims = (((1,), (1,)), ((), ()))
    return (lax.dot_general(hi, hi, dims, preferred_element_type=jnp.float32),
            lax.dot_general(hi, lo, dims, preferred_element_type=jnp.float32))


def lane_sum(x, mask):
    return jnp.broadcast_to(jnp.sum(jnp.where(mask, x, 0.0), axis=1, keepdims=True), x.shape)


def eliminate(d, base, lane, sub):
    n = SUBLANES
    cols = [lane_sum(d, lane == base + b) for b in range(n)]
    block = {(a, b): jnp.broadcast_to(cols[b][a : a + 1, :], d.shape) for b in range(n) for a in range(b + 1)}
    panel = (lane >= base) & (lane < base + n)
    rows = [jnp.where(panel, jnp.where(lane == base + a, 1.0, 0.0), jnp.broadcast_to(d[a : a + 1, :], d.shape))
            for a in range(n)]
    ratio, inverse = {}, []
    for a in range(n):
        inverse.append(1.0 / block[a, a])
        for b in range(a + 1, n):
            ratio[a, b] = block[a, b] * inverse[a]
            for c in range(b, n):
                block[b, c] = block[b, c] - ratio[a, b] * block[a, c]
            rows[b] = rows[b] - ratio[a, b] * rows[a]
    back = [None] * n
    for a in range(n - 1, -1, -1):
        back[a] = rows[a] * inverse[a]
        for c in range(a + 1, n):
            back[a] = back[a] - ratio[a, c] * back[c]
    packed, pivots = rows[0], block[0, 0]
    for a in range(1, n):
        packed = jnp.where(sub == a, rows[a], packed)
        pivots = jnp.where(sub == a, block[a, a], pivots)
    own = jnp.zeros_like(d)
    for b in range(n):
        col = block[0, b]
        for a in range(1, b + 1):
            col = jnp.where(sub == a, block[a, b], col)
        own = jnp.where((lane == base + b) & (sub <= b), col, own)
    scale = lax.rsqrt(pivots)
    left = lane < base + n
    return panel, back, jnp.where(left, packed, 0.0) * scale, jnp.where(left, own, packed) * scale


def factor(sums_ref, nrows, k, work, inverse_ref, upper_ref):
    width = work.shape[1]
    lane = lax.broadcasted_iota(jnp.int32, (SUBLANES, width), 1)
    sub = lax.broadcasted_iota(jnp.int32, (SUBLANES, width), 0)
    work[...] = sums_ref[...] * (1.0 / nrows)

    def step(first, i, carry):
        base = i * SUBLANES
        at = pl.ds(pl.multiple_of(base, SUBLANES), SUBLANES)
        panel, back, inverse_ref[at, :], upper_ref[at, :] = eliminate(work[at, :], base, lane, sub)
        for g in range(first, width // SUBLANES):
            w = work[g * SUBLANES : (g + 1) * SUBLANES, :]
            rest = jnp.where(panel, 0.0, w)
            for b in range(SUBLANES):
                rest = rest - lane_sum(w, lane == base + b) * back[b]
            work[g * SUBLANES : (g + 1) * SUBLANES, :] = rest
        return carry

    steps = k // SUBLANES
    mid = (steps + 1) // 2
    lax.fori_loop(0, mid, functools.partial(step, 1), 0)
    lax.fori_loop(mid, steps, functools.partial(step, mid + 1), 0)
    return work[k : k + SUBLANES, :]


def restart_kernel(ndev, ns, count, nrows, chunk, raw, u_hbm, r_hbm, restart_hbm, coeff_hbm,
                   big, small, coeff_out, u_ref, r_ref, restart_ref, coeff_ref, part, gathered, mine_ref, other_ref, red, sums, work, inverse, upper, weights_ref,
                   send, row_send, turn_send, turn_mid, turn_all, raw_ref, load_sem, own_sem,
                   s1, r1, s2, r2, s3, r3, s4, r4, s5, r5, s6, r6, s7, r7):
    r, s = lax.axis_index("rows"), lax.axis_index("sub")
    me = r * ns + s
    nr = ndev // ns
    keep, k = restart_ref.shape
    bs = send.shape[2]
    deg, mloc, _ = coeff_ref.shape
    pieces = u_ref.shape[1] // chunk

    def remote(src, dst, send_sem, recv_sem, dev):
        return pltpu.make_async_remote_copy(
            src_ref=src, dst_ref=dst, send_sem=send_sem, recv_sem=recv_sem, device_id=dev, device_id_type=MESH)

    def others(action):
        def body(o, carry):
            action((me + o) % ndev)
            return carry
        lax.fori_loop(1, ndev, body, 0)

    load_r = pltpu.make_async_copy(r_hbm, r_ref, load_sem.at[pieces])
    load_r.start()
    load_small = [pltpu.make_async_copy(restart_hbm, restart_ref, own_sem.at[0]),
                  pltpu.make_async_copy(coeff_hbm, coeff_ref, own_sem.at[1])]
    loads = []
    for c in range(pieces):
        cols = pl.ds(c * chunk, chunk)
        loads.append(pltpu.make_async_copy(u_hbm.at[:, cols], u_ref.at[:, cols], load_sem.at[c]))
        loads[-1].start()
    for load in load_small:
        load.start()
    barrier = greet_all(me, ndev, ns)

    half = ns // 2
    inner = (s == half - 1) | (s == half)
    facing = ns - 1 - s

    def raw_peer(q):
        return (r // 2 * 2 + (r + q) % 2 + q // 2 * 2) % nr

    def raw_source(q):
        return (r // 2 * 2 + (r + q) % 2 - q // 2 * 2 + nr) % nr

    def raw_copy(q):
        t = raw_peer(q)
        cols = pl.ds(pl.multiple_of((t * ns + facing) * bs, LANES), bs)
        return remote(u_hbm.at[:, cols], raw_ref.at[q], s7.at[q], r7.at[q], (t, facing))

    def for_raw(sender, action):
        for q in range(raw[0]):
            if q < raw[1]:
                action(q)
            else:
                @pl.when(sender(q) % 2 == 0)
                def _():
                    action(q)

    def raw_start():
        for_raw(lambda q: r, lambda q: raw_copy(q).start())

    def is_raw(j, peer, sender):
        hit = j < 0
        for q in range(raw[0]):
            one = j == peer(q) * ns + facing
            hit = hit | (one if q < raw[1] else one & (sender(q) % 2 == 0))
        return inner & hit

    def sent_raw(j):
        return is_raw(j, raw_peer, lambda q: r)

    def came_raw(j):
        return is_raw(j, raw_source, raw_source)

    load_r.wait()
    main = jnp.zeros((LANES, LANES), jnp.float32)
    cross = jnp.zeros((LANES, LANES), jnp.float32)
    for c in range(pieces):
        loads[c].wait()
        one, two = gram_piece(u_ref, r_ref, c * chunk, chunk)
        main = main + one
        cross = cross + two
        if c == min(RAW_AFTER, pieces - 1):
            pl.semaphore_wait(barrier, ndev - 1)

            @pl.when(inner & (r % 2 == 0))
            def _():
                raw_start()

    part[...] = main + (cross + cross.T)

    side, pos = s // half, s % half
    here = r * half + pos
    size = red.shape[0]
    groups = part.shape[0] // size
    own = (r // 2) * half + pos
    owning = (r % 2 == 1) & (own < groups)
    opposite = (r, (s + half) % ns)

    def member(m):
        return m // half, side * half + m % half

    def owner(g):
        return 2 * (g // half) + 1, side * half + g % half

    def group_rows(ref, g):
        return ref.at[pl.ds(pl.multiple_of(g * size, size), size), :]

    def scatter_copy(g, slot):
        return remote(group_rows(part, g), gathered.at[slot], s1.at[g], r1.at[slot], owner(g))

    def cross_copy():
        return remote(mine_ref, other_ref, s2.at[nr * half], r2.at[groups], opposite)

    def gather_copy(m, g):
        return remote(red, group_rows(sums, g), s2.at[m], r2.at[g], member(m))

    def groups_not_mine(action):
        def body(o, carry):
            g = (r // 2 * half + o) % groups
            @pl.when(jnp.logical_not(owning & (g == own)))
            def _():
                action(g)
            return carry
        lax.fori_loop(0, groups, body, 0)

    def half_others(action):
        def body(o, carry):
            action((here + o) % (nr * half))
            return carry
        lax.fori_loop(1, nr * half, body, 0)

    groups_not_mine(lambda g: scatter_copy(g, here).start())

    @pl.when(inner & (r % 2 == 1) & jnp.logical_not(owning))
    def _():
        raw_start()

    @pl.when(owning)
    def _():
        mine = pl.ds(pl.multiple_of(own * size, size), size)
        half_others(lambda m: scatter_copy(own, m).wait_recv())
        gathered[here] = part[mine, :]
        total = jnp.sum(gathered[...], axis=0)
        mine_ref[...] = total
        cross_copy().start()

        @pl.when(inner)
        def _():
            raw_start()

        cross_copy().wait_recv()
        total = total + other_ref[...]
        red[...] = total
        sums[mine, :] = total
        half_others(lambda m: gather_copy(m, own).start())

    groups_not_mine(lambda g: gather_copy(here, g).wait_recv())

    for load in load_small:
        load.wait()
    last = factor(sums, nrows, k, work, inverse, upper)
    weights_ref[:keep, :] = jnp.dot(restart_ref[...], inverse[...], precision=HIGHEST,
                                    preferred_element_type=jnp.float32)[:, :k]
    weights_ref[keep:, :] = -last[:, :k]

    def big_copy(j, slot):
        return remote(send.at[j], big.at[slot], s3.at[j], r3.at[slot], (j // ns, j % ns))

    def small_copy(j, slot):
        return remote(row_send.at[j], small.at[slot], s4.at[j], r4.at[slot], (j // ns, j % ns))

    across = [(1 - side) * half + (pos + q) % half for q in range(half)]
    beside = [side * half + (pos + q) % half for q in range(half)]
    order = []
    for q in range(half):
        order += [(across[q], True), (beside[half - 1 - q], False)]

    def project(j, acc):
        cols = pl.ds(pl.multiple_of(j * bs, bs), bs)
        y = jnp.dot(weights_ref[...], u_ref[:, cols], precision=HIGHEST, preferred_element_type=jnp.float32)
        rest = r_ref[:, cols] - y[keep : keep + 1, :]
        row_send[j, 0:1, :bs] = rest
        return y[:keep, :], acc + rest * rest

    def send_block(j, is_across):
        if is_across:
            @pl.when(jnp.logical_not(sent_raw(j)))
            def _():
                big_copy(j, me).start()
        else:
            big_copy(j, me).start()

    def step(d, acc):
        for t, is_across in order:
            j = ((r + d) % nr) * ns + t
            send[j], acc = project(j, acc)
            send_block(j, is_across)
        return acc

    def hold(d, acc):
        for t, _ in order:
            j = ((r + d) % nr) * ns + t
            send[j], acc = project(j, acc)
        return acc

    def release(d, carry):
        for t, is_across in order:
            send_block(((r + d) % nr) * ns + t, is_across)
        return carry

    acc = step(1, jnp.zeros((1, bs), jnp.float32))

    raised = jnp.dot(restart_ref[...], upper[...], precision=HIGHEST, preferred_element_type=jnp.float32)[:, :k]
    turn_send[...] = jnp.zeros_like(turn_send)
    for i in range(deg):
        turned = lax.dot_general(coeff_ref[i], raised, (((1,), (1,)), ((), ())), precision=HIGHEST,
                                 preferred_element_type=jnp.float32)
        turn_send[:mloc, i * keep : (i + 1) * keep] = turned
    share = turn_mid.shape[1]
    my_rows = pl.ds(pl.multiple_of(r * share, share), share)
    for i in range(nr):
        @pl.when(r == i)
        def _():
            turn_mid[s] = turn_send[i * share : (i + 1) * share, :]

    def turn_copy(t, slot):
        return remote(turn_mid.at[s], turn_mid.at[slot], s5.at[t], r5.at[slot], (r, t))

    def spread_copy(p, slot):
        return remote(turn_mid, turn_all.at[slot], s6.at[p], r6.at[slot], (p, s))

    def along(action):
        for o in range(1, ns):
            action((s + o) % ns)

    def plane(action):
        def body(o, carry):
            action((r + o) % nr)
            return carry
        lax.fori_loop(1, nr, body, 0)

    along(lambda t: turn_copy(t, s).start())
    held = min(nr, HELD_FROM)
    acc = lax.fori_loop(2, held, step, acc)
    acc = lax.fori_loop(held, nr, hold, acc)
    for t, _ in order[:-1]:
        j = r * ns + t
        send[j], acc = project(j, acc)
    big[me], acc = project(me, acc)
    partial = jnp.sum(acc, axis=1, keepdims=True)

    def mark(j, carry):
        row_send[j, 0:1, bs:] = jnp.broadcast_to(partial, (1, LANES))
        return carry

    lax.fori_loop(0, ndev, mark, 0)
    others(lambda j: small_copy(j, me).start())
    lax.fori_loop(held, nr, release, 0)
    for t, is_across in order[:-1]:
        send_block(r * ns + t, is_across)
    small[me] = row_send[me]

    @pl.when(inner)
    def _():
        def finish(q):
            raw_copy(q).wait_recv()
            y = jnp.dot(weights_ref[:keep, :], raw_ref[q], precision=HIGHEST, preferred_element_type=jnp.float32)
            big[raw_source(q) * ns + facing] = y
        for_raw(raw_source, finish)

    along(lambda t: turn_copy(t, t).wait_recv())
    plane(lambda p: spread_copy(p, r).start())
    turn_all[r] = turn_mid[...]
    plane(lambda p: spread_copy(p, p).wait_recv())
    columns = []
    for t in range(ns):
        columns.append(jnp.concatenate([turn_all[p, t] for p in range(nr)], axis=0)[:mloc, :])
    turned = jnp.concatenate(columns, axis=0).T
    squares = jnp.sum(turned * turned)
    scale = lax.rsqrt(jnp.full((1, 1), squares / count + 1e-06, jnp.float32))
    for i in range(deg):
        coeff_out[i] = turned[i * keep : (i + 1) * keep, :] * scale

    def others_cooked(skip, action):
        def body(j):
            @pl.when(jnp.logical_not(skip(j)))
            def _():
                action(j)
        others(body)

    others_cooked(came_raw, lambda j: big_copy(j, j).wait_recv())
    others(lambda j: small_copy(j, j).wait_recv())
    groups_not_mine(lambda g: scatter_copy(g, here).wait_send())

    @pl.when(owning)
    def _():
        cross_copy().wait_send()
        half_others(lambda m: gather_copy(m, own).wait_send())

    @pl.when(inner)
    def _():
        for_raw(lambda q: r, lambda q: raw_copy(q).wait_send())

    others_cooked(sent_raw, lambda j: big_copy(j, me).wait_send())
    others(lambda j: small_copy(j, me).wait_send())
    along(lambda t: turn_copy(t, s).wait_send())
    plane(lambda p: spread_copy(p, r).wait_send())


def restart_call(u, r, restart, coeff_t, ndev, ns):
    f32 = jnp.float32
    bs = u.shape[1] // ndev
    nr = ndev // ns
    keep, k = restart.shape
    deg, mloc, _ = coeff_t.shape
    count = deg * keep * mloc * ns
    chunk = min(2048, u.shape[1])
    size = 2 * SUBLANES
    groups = LANES // size
    share = -(-mloc // nr)
    lanes = -(-deg * keep // LANES) * LANES
    vmem = pl.BlockSpec(memory_space=pltpu.VMEM)
    hbm = pl.BlockSpec(memory_space=pltpu.MemorySpace.HBM)
    dma = pltpu.SemaphoreType.DMA
    return pl.pallas_call(
        functools.partial(restart_kernel, ndev, ns, count, u.shape[1] * ndev, chunk, RAW_BLOCKS),
        out_shape=(
            pltpu.VMEM((ndev, keep, bs), f32),
            pltpu.VMEM((ndev, 1, bs + LANES), f32),
            pltpu.VMEM((deg, keep, ns * mloc), f32),
        ),
        in_specs=[hbm, hbm, hbm, hbm],
        out_specs=(vmem, vmem, vmem),
        scratch_shapes=[
            pltpu.VMEM(u.shape, f32),
            pltpu.VMEM(r.shape, f32),
            pltpu.VMEM(restart.shape, f32),
            pltpu.VMEM(coeff_t.shape, f32),
            pltpu.VMEM((LANES, LANES), f32),
            pltpu.VMEM((ndev // 2, size, LANES), f32),
            pltpu.VMEM((size, LANES), f32),
            pltpu.VMEM((size, LANES), f32),
            pltpu.VMEM((size, LANES), f32),
            pltpu.VMEM((LANES, LANES), f32),
            pltpu.VMEM((LANES, LANES), f32),
            pltpu.VMEM((k, LANES), f32),
            pltpu.VMEM((k, LANES), f32),
            pltpu.VMEM((keep + SUBLANES, k), f32),
            pltpu.VMEM((ndev, keep, bs), f32),
            pltpu.VMEM((ndev, 1, bs + LANES), f32),
            pltpu.VMEM((nr * share, lanes), f32),
            pltpu.VMEM((ns, share, lanes), f32),
            pltpu.VMEM((nr, ns, share, lanes), f32),
            pltpu.VMEM((RAW_BLOCKS[0], k, bs), f32),
            dma((u.shape[1] // chunk + 1,)),
            dma((2,)),
            dma((groups,)), dma((ndev // 2,)),
            dma((ndev // 2 + 1,)), dma((groups + 1,)),
            dma((ndev,)), dma((ndev,)),
            dma((ndev,)), dma((ndev,)),
            dma((ns,)), dma((ns,)),
            dma((nr,)), dma((nr,)),
            dma((RAW_BLOCKS[0],)), dma((RAW_BLOCKS[0],)),
        ],
        compiler_params=pltpu.CompilerParams(
            collective_id=0, has_side_effects=True, vmem_limit_bytes=48 * 1024 * 1024),
    )(*[pltpu.with_memory_space_constraint(a, pltpu.MemorySpace.HBM) for a in (u, r, restart, coeff_t)])


def place_kernel(ndev, nrows, slots, big, small, coeff, rows_out, vec_out, coeff_out, vec, out_sem, side_sem):
    bs = big.shape[2]

    def put(d):
        cols = pl.ds(pl.multiple_of(slots[0, d] * bs, bs), bs)
        return pltpu.make_async_copy(big.at[d], rows_out.at[:, cols], out_sem.at[d])

    def loop(action):
        def body(d, carry):
            action(d)
            return carry
        lax.fori_loop(0, ndev, body, 0)

    loop(lambda d: put(d).start())
    put_coeff = pltpu.make_async_copy(coeff, coeff_out, side_sem.at[0])
    put_coeff.start()
    total = jnp.sum(small[:, 0, bs : bs + LANES], axis=0, keepdims=True)[:, :1]
    scale = lax.rsqrt(total / nrows + 1e-06)
    for d in range(ndev):
        cols = pl.ds(pl.multiple_of(slots[0, d] * bs, bs), bs)
        vec[:, cols] = small[d, 0:1, :bs] * scale
    put_vec = pltpu.make_async_copy(vec, vec_out, side_sem.at[1])
    put_vec.start()
    loop(lambda d: put(d).wait())
    put_coeff.wait()
    put_vec.wait()


def place(slot_row, big, small, coeff, nrows):
    ndev, keep, bs = big.shape
    vmem = pl.BlockSpec(memory_space=pltpu.VMEM)
    hbm = pl.BlockSpec(memory_space=pltpu.MemorySpace.HBM)
    return pl.pallas_call(
        functools.partial(place_kernel, ndev, nrows),
        out_shape=(
            jax.ShapeDtypeStruct((keep, ndev * bs), jnp.float32),
            jax.ShapeDtypeStruct((1, ndev * bs), jnp.float32),
            jax.ShapeDtypeStruct(coeff.shape, jnp.float32),
        ),
        in_specs=[pl.BlockSpec(memory_space=pltpu.SMEM), vmem, vmem, vmem],
        out_specs=(hbm, hbm, hbm),
        scratch_shapes=[pltpu.VMEM((1, ndev * bs), jnp.float32), pltpu.SemaphoreType.DMA((ndev,)),
                        pltpu.SemaphoreType.DMA((2,))],
        compiler_params=pltpu.CompilerParams(vmem_limit_bytes=32 * 1024 * 1024),
    )(slot_row, big, small, coeff)


def local(u, r, slot_map, restart, coeff):
    ndev = lax.axis_size(AXES)
    ns = lax.axis_size("sub")
    nrows = u.shape[1] * ndev
    big, small, new_coeff = restart_call(u, r, restart.T, coeff.transpose(0, 2, 1), ndev, ns)
    return place(slot_map, big, small, new_coeff, nrows)


def solution(mesh):
    P = jax.sharding.PartitionSpec
    in_specs = (P(None, AXES), P(None, AXES), P(AXES, None), P(), P(None, None, "sub"))
    out_specs = (P(None, AXES), P(None, AXES), P())
    return jax.shard_map(local, mesh=mesh, in_specs=in_specs, out_specs=out_specs, check_vma=False)
```

```python
import functools

import jax
import jax.numpy as jnp
from jax import lax
from jax.experimental import pallas as pl
from jax.experimental.pallas import tpu as pltpu

HIGHEST = lax.Precision.HIGHEST
MESH = pl.DeviceIdType.MESH
AXES = ("rows", "sub")
LANES = 128
SUBLANES = 8
RAW_BLOCKS = (3, 2)
RAW_AFTER = 5
HELD_FROM = 4


def greet_all(me, ndev, ns):
    barrier = pltpu.get_barrier_semaphore()

    def greet(o, carry):
        j = (me + o) % ndev
        pl.semaphore_signal(barrier, inc=1, device_id=(j // ns, j % ns), device_id_type=MESH)
        return carry

    lax.fori_loop(1, ndev, greet, 0)
    return barrier


def gram_piece(u_ref, r_ref, col, chunk):
    cols = pl.ds(col, chunk)
    pad = LANES - u_ref.shape[0]
    first = lax.broadcasted_iota(jnp.int32, (pad, chunk), 0) == 0
    tail = jnp.where(first, jnp.broadcast_to(r_ref[:, cols], (pad, chunk)), 0.0)
    x = jnp.concatenate([u_ref[:, cols], tail], axis=0)
    hi = x.astype(jnp.bfloat16)
    lo = (x - hi.astype(jnp.float32)).astype(jnp.bfloat16)
    dims = (((1,), (1,)), ((), ()))
    return (lax.dot_general(hi, hi, dims, preferred_element_type=jnp.float32),
            lax.dot_general(lo, hi, dims, preferred_element_type=jnp.float32))


def lane_sum(x, mask):
    return jnp.broadcast_to(jnp.sum(jnp.where(mask, x, 0.0), axis=1, keepdims=True), x.shape)


def eliminate(d, base, lane, sub):
    n = SUBLANES
    cols = [lane_sum(d, lane == base + b) for b in range(n)]
    block = {(a, b): jnp.broadcast_to(cols[b][a : a + 1, :], d.shape) for b in range(n) for a in range(b + 1)}
    panel = (lane >= base) & (lane < base + n)
    rows = [jnp.where(panel, jnp.where(lane == base + a, 1.0, 0.0), jnp.broadcast_to(d[a : a + 1, :], d.shape))
            for a in range(n)]
    ratio, inverse = {}, []
    for a in range(n):
        inverse.append(1.0 / block[a, a])
        for b in range(a + 1, n):
            ratio[a, b] = block[a, b] * inverse[a]
            for c in range(b, n):
                block[b, c] = block[b, c] - ratio[a, b] * block[a, c]
            rows[b] = rows[b] - ratio[a, b] * rows[a]
    back = [None] * n
    for a in range(n - 1, -1, -1):
        back[a] = rows[a] * inverse[a]
        for c in range(a + 1, n):
            back[a] = back[a] - ratio[a, c] * back[c]
    packed, pivots = rows[0], block[0, 0]
    for a in range(1, n):
        packed = jnp.where(sub == a, rows[a], packed)
        pivots = jnp.where(sub == a, block[a, a], pivots)
    own = jnp.zeros_like(d)
    for b in range(n):
        col = block[0, b]
        for a in range(1, b + 1):
            col = jnp.where(sub == a, block[a, b], col)
        own = jnp.where((lane == base + b) & (sub <= b), col, own)
    scale = lax.rsqrt(pivots)
    left = lane < base + n
    return panel, back, jnp.where(left, packed, 0.0) * scale, jnp.where(left, own, packed) * scale


def factor(sums_ref, nrows, k, work, inverse_ref, upper_ref):
    width = work.shape[1]
    lane = lax.broadcasted_iota(jnp.int32, (SUBLANES, width), 1)
    sub = lax.broadcasted_iota(jnp.int32, (SUBLANES, width), 0)
    work[...] = sums_ref[...] * (1.0 / nrows)

    def step(first, i, carry):
        base = i * SUBLANES
        at = pl.ds(pl.multiple_of(base, SUBLANES), SUBLANES)
        panel, back, inverse_ref[at, :], upper_ref[at, :] = eliminate(work[at, :], base, lane, sub)
        for g in range(first, width // SUBLANES):
            w = work[g * SUBLANES : (g + 1) * SUBLANES, :]
            rest = jnp.where(panel, 0.0, w)
            for b in range(SUBLANES):
                rest = rest - lane_sum(w, lane == base + b) * back[b]
            work[g * SUBLANES : (g + 1) * SUBLANES, :] = rest
        return carry

    steps = k // SUBLANES
    mid = (steps + 1) // 2
    lax.fori_loop(0, mid, functools.partial(step, 1), 0)
    lax.fori_loop(mid, steps, functools.partial(step, mid + 1), 0)
    return work[k : k + SUBLANES, :]


def restart_kernel(ndev, ns, count, nrows, chunk, raw, u_hbm, r_hbm, restart_hbm, coeff_hbm,
                   big, small, coeff_out, u_ref, r_ref, restart_ref, coeff_ref, part, gathered, mine_ref, other_ref, red, sums, work, inverse, upper, weights_ref,
                   send, row_send, turn_send, turn_mid, turn_all, raw_ref, load_sem, own_sem,
                   s1, r1, s2, r2, s3, r3, s4, r4, s5, r5, s6, r6, s7, r7):
    r, s = lax.axis_index("rows"), lax.axis_index("sub")
    me = r * ns + s
    nr = ndev // ns
    keep, k = restart_ref.shape
    bs = send.shape[2]
    deg, mloc, _ = coeff_ref.shape
    pieces = u_ref.shape[1] // chunk

    def remote(src, dst, send_sem, recv_sem, dev):
        return pltpu.make_async_remote_copy(
            src_ref=src, dst_ref=dst, send_sem=send_sem, recv_sem=recv_sem, device_id=dev, device_id_type=MESH)

    def others(action):
        def body(o, carry):
            action((me + o) % ndev)
            return carry
        lax.fori_loop(1, ndev, body, 0)

    load_r = pltpu.make_async_copy(r_hbm, r_ref, load_sem.at[pieces])
    load_r.start()
    load_small = [pltpu.make_async_copy(restart_hbm, restart_ref, own_sem.at[0]),
                  pltpu.make_async_copy(coeff_hbm, coeff_ref, own_sem.at[1])]
    loads = []
    for c in range(pieces):
        cols = pl.ds(c * chunk, chunk)
        loads.append(pltpu.make_async_copy(u_hbm.at[:, cols], u_ref.at[:, cols], load_sem.at[c]))
        loads[-1].start()
    for load in load_small:
        load.start()
    barrier = greet_all(me, ndev, ns)

    half = ns // 2
    inner = (s == half - 1) | (s == half)
    facing = ns - 1 - s

    def raw_peer(q):
        pair = r // 2
        return (pair // 2 * 2 + (pair + q // 2) % 2) * 2 + (r + q) % 2

    def raw_source(q):
        return raw_peer(q)

    def raw_copy(q):
        t = raw_peer(q)
        cols = pl.ds(pl.multiple_of((t * ns + facing) * bs, LANES), bs)
        return remote(u_hbm.at[:, cols], raw_ref.at[q], s7.at[q], r7.at[q], (t, facing))

    def for_raw(sender, action):
        for q in range(raw[0]):
            if q < raw[1]:
                action(q)
            else:
                @pl.when(sender(q) % 2 == 0)
                def _():
                    action(q)

    def raw_start():
        for_raw(lambda q: r, lambda q: raw_copy(q).start())

    def is_raw(j, peer, sender):
        hit = j < 0
        for q in range(raw[0]):
            one = j == peer(q) * ns + facing
            hit = hit | (one if q < raw[1] else one & (sender(q) % 2 == 0))
        return inner & hit

    def sent_raw(j):
        return is_raw(j, raw_peer, lambda q: r)

    def came_raw(j):
        return is_raw(j, raw_source, raw_source)

    load_r.wait()
    main = jnp.zeros((LANES, LANES), jnp.float32)
    cross = jnp.zeros((LANES, LANES), jnp.float32)
    for c in range(pieces):
        loads[c].wait()
        one, two = gram_piece(u_ref, r_ref, c * chunk, chunk)
        main = main + one
        cross = cross + two
        if c == min(RAW_AFTER, pieces - 1):
            pl.semaphore_wait(barrier, ndev - 1)

            @pl.when(inner & (r % 2 == 0))
            def _():
                raw_start()

    part[...] = main + (cross + cross.T)

    side, pos = s // half, s % half
    here = r * half + pos
    size = red.shape[0]
    groups = part.shape[0] // size
    own = (r // 2) * half + pos
    owning = (r % 2 == 1) & (own < groups)
    opposite = (r, (s + half) % ns)

    def member(m):
        return m // half, side * half + m % half

    def owner(g):
        return 2 * (g // half) + 1, side * half + g % half

    def group_rows(ref, g):
        return ref.at[pl.ds(pl.multiple_of(g * size, size), size), :]

    def scatter_copy(g, slot):
        return remote(group_rows(part, g), gathered.at[slot], s1.at[g], r1.at[slot], owner(g))

    def cross_copy():
        return remote(mine_ref, other_ref, s2.at[nr * half], r2.at[groups], opposite)

    def gather_copy(m, g):
        return remote(red, group_rows(sums, g), s2.at[m], r2.at[g], member(m))

    def groups_not_mine(action):
        def body(o, carry):
            g = (r // 2 * half + o) % groups
            @pl.when(jnp.logical_not(owning & (g == own)))
            def _():
                action(g)
            return carry
        lax.fori_loop(0, groups, body, 0)

    def half_others(action):
        for o in range(1, nr * half):
            action((here + o) % (nr * half))

    groups_not_mine(lambda g: scatter_copy(g, here).start())

    @pl.when(inner & (r % 2 == 1) & jnp.logical_not(owning))
    def _():
        raw_start()

    @pl.when(owning)
    def _():
        mine = pl.ds(pl.multiple_of(own * size, size), size)
        half_others(lambda m: scatter_copy(own, m).wait_recv())
        gathered[here] = part[mine, :]
        total = jnp.sum(gathered[...], axis=0)
        mine_ref[...] = total
        cross_copy().start()

        @pl.when(inner)
        def _():
            raw_start()

        cross_copy().wait_recv()
        total = total + other_ref[...]
        red[...] = total
        sums[mine, :] = total
        half_others(lambda m: gather_copy(m, own).start())

    groups_not_mine(lambda g: gather_copy(here, g).wait_recv())

    for load in load_small:
        load.wait()
    last = factor(sums, nrows, k, work, inverse, upper)
    weights_ref[:keep, :] = jnp.dot(restart_ref[...], inverse[...], precision=HIGHEST,
                                    preferred_element_type=jnp.float32)[:, :k]
    weights_ref[keep:, :] = -last[:, :k]

    def big_copy(j, slot):
        return remote(send.at[j], big.at[slot], s3.at[j], r3.at[slot], (j // ns, j % ns))

    def small_copy(j, slot):
        return remote(row_send.at[j], small.at[slot], s4.at[j], r4.at[slot], (j // ns, j % ns))

    across = [(1 - side) * half + (pos + q) % half for q in range(half)]
    beside = [side * half + (pos + q) % half for q in range(half)]
    order = []
    for q in range(half):
        order += [(across[q], True), (beside[half - 1 - q], False)]

    def project(j, acc):
        cols = pl.ds(pl.multiple_of(j * bs, bs), bs)
        y = jnp.dot(weights_ref[...], u_ref[:, cols], precision=HIGHEST, preferred_element_type=jnp.float32)
        rest = r_ref[:, cols] - y[keep : keep + 1, :]
        row_send[j, 0:1, :bs] = rest
        return y[:keep, :], acc + rest * rest

    def send_block(j, is_across):
        if is_across:
            @pl.when(jnp.logical_not(sent_raw(j)))
            def _():
                big_copy(j, me).start()
        else:
            big_copy(j, me).start()

    def step(d, acc):
        for t, is_across in order:
            j = ((r + d) % nr) * ns + t
            send[j], acc = project(j, acc)
            send_block(j, is_across)
        return acc

    def hold(d, acc):
        for t, _ in order:
            j = ((r + d) % nr) * ns + t
            send[j], acc = project(j, acc)
        return acc

    def release(d, carry):
        for t, is_across in order:
            send_block(((r + d) % nr) * ns + t, is_across)
        return carry

    acc = step(1, jnp.zeros((1, bs), jnp.float32))

    raised = jnp.dot(restart_ref[...], upper[...], precision=HIGHEST, preferred_element_type=jnp.float32)[:, :k]
    turn_send[...] = jnp.zeros_like(turn_send)
    for i in range(deg):
        turned = lax.dot_general(coeff_ref[i], raised, (((1,), (1,)), ((), ())), precision=HIGHEST,
                                 preferred_element_type=jnp.float32)
        turn_send[:mloc, i * keep : (i + 1) * keep] = turned
    share = turn_mid.shape[1]
    my_rows = pl.ds(pl.multiple_of(r * share, share), share)
    for i in range(nr):
        @pl.when(r == i)
        def _():
            turn_mid[s] = turn_send[i * share : (i + 1) * share, :]

    def turn_copy(t, slot):
        return remote(turn_mid.at[s], turn_mid.at[slot], s5.at[t], r5.at[slot], (r, t))

    def spread_copy(p, slot):
        return remote(turn_mid, turn_all.at[slot], s6.at[p], r6.at[slot], (p, s))

    def along(action):
        for o in range(1, ns):
            action((s + o) % ns)

    def plane(action):
        def body(o, carry):
            action((r + o) % nr)
            return carry
        lax.fori_loop(1, nr, body, 0)

    along(lambda t: turn_copy(t, s).start())
    held = min(nr, HELD_FROM)
    acc = lax.fori_loop(2, held, step, acc)
    acc = lax.fori_loop(held, nr, hold, acc)
    for t, _ in order[:-1]:
        j = r * ns + t
        send[j], acc = project(j, acc)
    big[me], acc = project(me, acc)
    partial = jnp.sum(acc, axis=1, keepdims=True)

    def mark(j, carry):
        row_send[j, 0:1, bs:] = jnp.broadcast_to(partial, (1, LANES))
        return carry

    lax.fori_loop(0, ndev, mark, 0)
    others(lambda j: small_copy(j, me).start())
    lax.fori_loop(held, nr, release, 0)
    for t, is_across in order[:-1]:
        send_block(r * ns + t, is_across)
    small[me] = row_send[me]

    @pl.when(inner)
    def _():
        def finish(q):
            raw_copy(q).wait_recv()
            y = jnp.dot(weights_ref[:keep, :], raw_ref[q], precision=HIGHEST, preferred_element_type=jnp.float32)
            big[raw_source(q) * ns + facing] = y
        for_raw(raw_source, finish)

    along(lambda t: turn_copy(t, t).wait_recv())
    plane(lambda p: spread_copy(p, r).start())
    turn_all[r] = turn_mid[...]
    plane(lambda p: spread_copy(p, p).wait_recv())
    columns = []
    for t in range(ns):
        columns.append(jnp.concatenate([turn_all[p, t] for p in range(nr)], axis=0)[:mloc, :])
    turned = jnp.concatenate(columns, axis=0).T
    squares = jnp.sum(turned * turned)
    scale = lax.rsqrt(jnp.full((1, 1), squares / count + 1e-06, jnp.float32))
    for i in range(deg):
        coeff_out[i] = turned[i * keep : (i + 1) * keep, :] * scale

    def others_cooked(skip, action):
        def body(j):
            @pl.when(jnp.logical_not(skip(j)))
            def _():
                action(j)
        others(body)

    others_cooked(came_raw, lambda j: big_copy(j, j).wait_recv())
    others(lambda j: small_copy(j, j).wait_recv())
    groups_not_mine(lambda g: scatter_copy(g, here).wait_send())

    @pl.when(owning)
    def _():
        cross_copy().wait_send()
        half_others(lambda m: gather_copy(m, own).wait_send())

    @pl.when(inner)
    def _():
        for_raw(lambda q: r, lambda q: raw_copy(q).wait_send())

    others_cooked(sent_raw, lambda j: big_copy(j, me).wait_send())
    others(lambda j: small_copy(j, me).wait_send())
    along(lambda t: turn_copy(t, s).wait_send())
    plane(lambda p: spread_copy(p, r).wait_send())


def restart_call(u, r, restart, coeff_t, ndev, ns):
    f32 = jnp.float32
    bs = u.shape[1] // ndev
    nr = ndev // ns
    keep, k = restart.shape
    deg, mloc, _ = coeff_t.shape
    count = deg * keep * mloc * ns
    chunk = min(2048, u.shape[1])
    size = 2 * SUBLANES
    groups = LANES // size
    share = -(-mloc // nr)
    lanes = -(-deg * keep // LANES) * LANES
    vmem = pl.BlockSpec(memory_space=pltpu.VMEM)
    hbm = pl.BlockSpec(memory_space=pltpu.MemorySpace.HBM)
    dma = pltpu.SemaphoreType.DMA
    return pl.pallas_call(
        functools.partial(restart_kernel, ndev, ns, count, u.shape[1] * ndev, chunk, RAW_BLOCKS),
        out_shape=(
            pltpu.VMEM((ndev, keep, bs), f32),
            pltpu.VMEM((ndev, 1, bs + LANES), f32),
            pltpu.VMEM((deg, keep, ns * mloc), f32),
        ),
        in_specs=[hbm, hbm, hbm, hbm],
        out_specs=(vmem, vmem, vmem),
        scratch_shapes=[
            pltpu.VMEM(u.shape, f32),
            pltpu.VMEM(r.shape, f32),
            pltpu.VMEM(restart.shape, f32),
            pltpu.VMEM(coeff_t.shape, f32),
            pltpu.VMEM((LANES, LANES), f32),
            pltpu.VMEM((ndev // 2, size, LANES), f32),
            pltpu.VMEM((size, LANES), f32),
            pltpu.VMEM((size, LANES), f32),
            pltpu.VMEM((size, LANES), f32),
            pltpu.VMEM((LANES, LANES), f32),
            pltpu.VMEM((LANES, LANES), f32),
            pltpu.VMEM((k, LANES), f32),
            pltpu.VMEM((k, LANES), f32),
            pltpu.VMEM((keep + SUBLANES, k), f32),
            pltpu.VMEM((ndev, keep, bs), f32),
            pltpu.VMEM((ndev, 1, bs + LANES), f32),
            pltpu.VMEM((nr * share, lanes), f32),
            pltpu.VMEM((ns, share, lanes), f32),
            pltpu.VMEM((nr, ns, share, lanes), f32),
            pltpu.VMEM((RAW_BLOCKS[0], k, bs), f32),
            dma((u.shape[1] // chunk + 1,)),
            dma((2,)),
            dma((groups,)), dma((ndev // 2,)),
            dma((ndev // 2 + 1,)), dma((groups + 1,)),
            dma((ndev,)), dma((ndev,)),
            dma((ndev,)), dma((ndev,)),
            dma((ns,)), dma((ns,)),
            dma((nr,)), dma((nr,)),
            dma((RAW_BLOCKS[0],)), dma((RAW_BLOCKS[0],)),
        ],
        compiler_params=pltpu.CompilerParams(
            collective_id=0, has_side_effects=True, vmem_limit_bytes=48 * 1024 * 1024),
    )(*[pltpu.with_memory_space_constraint(a, pltpu.MemorySpace.HBM) for a in (u, r, restart, coeff_t)])


def place_kernel(ndev, nrows, slots, big, small, coeff, rows_out, vec_out, coeff_out, vec, out_sem, side_sem):
    bs = big.shape[2]

    def put(d):
        cols = pl.ds(pl.multiple_of(slots[0, d] * bs, bs), bs)
        return pltpu.make_async_copy(big.at[d], rows_out.at[:, cols], out_sem.at[d])

    def loop(action):
        def body(d, carry):
            action(d)
            return carry
        lax.fori_loop(0, ndev, body, 0)

    loop(lambda d: put(d).start())
    put_coeff = pltpu.make_async_copy(coeff, coeff_out, side_sem.at[0])
    put_coeff.start()
    total = jnp.sum(small[:, 0, bs : bs + LANES], axis=0, keepdims=True)[:, :1]
    scale = lax.rsqrt(total / nrows + 1e-06)
    for d in range(ndev):
        cols = pl.ds(pl.multiple_of(slots[0, d] * bs, bs), bs)
        vec[:, cols] = small[d, 0:1, :bs] * scale
    put_vec = pltpu.make_async_copy(vec, vec_out, side_sem.at[1])
    put_vec.start()
    loop(lambda d: put(d).wait())
    put_coeff.wait()
    put_vec.wait()


def place(slot_row, big, small, coeff, nrows):
    ndev, keep, bs = big.shape
    vmem = pl.BlockSpec(memory_space=pltpu.VMEM)
    hbm = pl.BlockSpec(memory_space=pltpu.MemorySpace.HBM)
    return pl.pallas_call(
        functools.partial(place_kernel, ndev, nrows),
        out_shape=(
            jax.ShapeDtypeStruct((keep, ndev * bs), jnp.float32),
            jax.ShapeDtypeStruct((1, ndev * bs), jnp.float32),
            jax.ShapeDtypeStruct(coeff.shape, jnp.float32),
        ),
        in_specs=[pl.BlockSpec(memory_space=pltpu.SMEM), vmem, vmem, vmem],
        out_specs=(hbm, hbm, hbm),
        scratch_shapes=[pltpu.VMEM((1, ndev * bs), jnp.float32), pltpu.SemaphoreType.DMA((ndev,)),
                        pltpu.SemaphoreType.DMA((2,))],
        compiler_params=pltpu.CompilerParams(vmem_limit_bytes=32 * 1024 * 1024),
    )(slot_row, big, small, coeff)


def local(u, r, slot_map, restart, coeff):
    ndev = lax.axis_size(AXES)
    ns = lax.axis_size("sub")
    nrows = u.shape[1] * ndev
    big, small, new_coeff = restart_call(u, r, restart.T, coeff.transpose(0, 2, 1), ndev, ns)
    return place(slot_map, big, small, new_coeff, nrows)


def solution(mesh):
    P = jax.sharding.PartitionSpec
    in_specs = (P(None, AXES), P(None, AXES), P(AXES, None), P(), P(None, None, "sub"))
    out_specs = (P(None, AXES), P(None, AXES), P())
    return jax.shard_map(local, mesh=mesh, in_specs=in_specs, out_specs=out_specs, check_vma=False)
```
